32 devices in a mesh: depth: 8 (over y, x, core), screen: 4 (over z).
Axes of the slice: x: 2, y: 2, z: 4, core: 2. Of those that a mesh axis runs over, the one named last changes fastest.
Arguments:
- block_tile: int32 [8, 8192], P('depth', 'screen'), may hold values from 0 to 127
- block_count: int32 [8, 4], P('depth', 'screen'), may hold values from 256 to 2048, as said below
- slab_rank: int32 [8], replicated, may hold values from 0 to 7, each once
- corner: int32 [2, 8, 8192, 128], P(None, 'depth', 'screen'), may hold values from 0 to 16
- offset: float32 [2, 8, 8192, 128], P(None, 'depth', 'screen'), may hold values from 0.25 to 0.75
- radius: float32 [8, 8192, 128], P('depth', 'screen'), may hold values from 3 to 8
- emission: float32 [3, 8, 8192, 128], P(None, 'depth', 'screen'), may hold values from 0.002 to 0.02
- extinction: float32 [8, 8192, 128], P('depth', 'screen'), may hold values from 0.001 to 0.01
Outputs:
- image_tiles: float32 [128, 32, 128], P(('depth', 'screen'))
The draws below stay inside these ranges and needn't reach their ends.
Inputs may be any that keep to these rules, and one draw needn't show every extreme that they name: The live slots of a device are its first block_count slots; one device of every draw has all 2048 slots live. `block_tile`: a block holds particles of one tile. `corner`: a footprint box lies inside its tile. `slab_rank`: each slab once.
All inputs are finite; a program needn't handle non-finite values.
Results may differ from the reference program's by a relative error of at most 0.0003.
Values sent between devices are 32-bit elements; how exact they have to be, the bound alone decides.
A program may use at most 128 MiB of HBM per device.

```python
import math
import jax
import jax.numpy as jnp
import numpy as np
from jax import lax

TS = 32
FOOT = 16
PB = 128
BLK_DEV = 2048
TILES = 128
N_DEPTH = 8
N_SCREEN = 4


def draw_block_count(key, part):
    counts = jax.random.randint(key, (N_DEPTH, N_SCREEN), max(1, BLK_DEV // 8), BLK_DEV // 2 + 1)
    fullest = jax.random.randint(jax.random.fold_in(key, 7), (), 0, N_DEPTH * N_SCREEN)
    flattened = jnp.where(jnp.arange(N_DEPTH * N_SCREEN) == fullest, BLK_DEV, counts.reshape(-1))
    return flattened.reshape(N_DEPTH, N_SCREEN).astype(jnp.int32)


def place_ends(values, rng, low, high):
    shape = values.shape
    index_at = [jax.random.randint(jax.random.fold_in(rng, axis), (), 0, shape[axis]) for axis in range(len(shape))]
    values = values.at[tuple(index_at)].set(low)
    longest = shape.index(max(shape))
    index_at[longest] = (index_at[longest] + 1) % shape[longest]
    return values.at[tuple(index_at)].set(high)


def block_levels(rng, shape, cuts, low, high):
    factor_of = 1.0
    for axis_at, parts in cuts:
        steps = jax.random.uniform(jax.random.fold_in(jax.random.fold_in(rng, 6), axis_at), (parts,), jnp.float32, low / len(cuts), high / len(cuts))
        factor_of = factor_of * jnp.repeat(jnp.exp(steps), shape[axis_at] // parts).reshape((-1,) + (1,) * (len(shape) - 1 - axis_at))
    return factor_of


def rank_table(count, lean):
    loads = [(1 << 20) // math.isqrt(rank ** lean) + 1 for rank in range(1, count + 1)]
    scale = 1 + sum(loads) // (1 << 30)
    return np.cumsum(np.array([max(1, weight // scale) for weight in loads]))


def ranked(rng, dims, amount, slope):
    table = rank_table(amount, slope)
    pick = jax.random.randint(jax.random.fold_in(rng, 1), dims, 0, int(table[amount - 1]))
    grade = jnp.searchsorted(jnp.asarray(table, jnp.int32), pick, side="right")
    return jax.random.permutation(jax.random.fold_in(rng, 2), amount)[grade].astype(jnp.int32)


def setup_inputs(seed: int = 0) -> dict:
    seeds = jax.random.split(jax.random.key(seed), 9)
    return {
        "block_tile": place_ends(ranked(seeds[0], (N_DEPTH, N_SCREEN * BLK_DEV), TILES, 1), jax.random.fold_in(seeds[0], 3), 0, TILES - 1).astype(jnp.int32),
        "block_count": draw_block_count(jax.random.fold_in(seeds[8], 71), 0),
        "slab_rank": jax.random.permutation(seeds[2], N_DEPTH).astype(jnp.int32),
        "corner": place_ends(jax.random.randint(seeds[3], (2, N_DEPTH, N_SCREEN * BLK_DEV, PB), 0, TS - FOOT + 1), jax.random.fold_in(seeds[3], 1), 0, TS - FOOT).astype(jnp.int32),
        "offset": jnp.clip(0.25 + 0.5 * jax.random.uniform(seeds[4], (2, N_DEPTH, N_SCREEN * BLK_DEV, PB), jnp.float32) ** block_levels(seeds[4], (2, N_DEPTH, N_SCREEN * BLK_DEV, PB), ((1, 8), (2, 4)), -0.2, 0.2), 0.25, 0.75),
        "radius": jnp.clip(3.0 + 5.0 * jax.random.uniform(seeds[5], (N_DEPTH, N_SCREEN * BLK_DEV, PB), jnp.float32) ** block_levels(seeds[5], (N_DEPTH, N_SCREEN * BLK_DEV, PB), ((0, 8), (1, 4)), -0.2, 0.2), 3.0, 8.0),
        "emission": jnp.clip(jnp.exp(math.log(0.02) - 2.30258502 * jax.random.uniform(seeds[6], (3, N_DEPTH, N_SCREEN * BLK_DEV, PB), jnp.float32) ** block_levels(seeds[6], (3, N_DEPTH, N_SCREEN * BLK_DEV, PB), ((1, 8), (2, 4)), -0.2, 0.2)), 0.002, 0.02),
        "extinction": jnp.clip(jnp.exp(math.log(0.01) - 2.30258502 * jax.random.uniform(seeds[7], (N_DEPTH, N_SCREEN * BLK_DEV, PB), jnp.float32) ** block_levels(seeds[7], (N_DEPTH, N_SCREEN * BLK_DEV, PB), ((0, 8), (1, 4)), -0.2, 0.2)), 0.001, 0.01),
    }


def axis_weights(corner, offset, radius, tile_side, foot):
    pixel_index = jnp.arange(tile_side, dtype=jnp.int32)
    pixel_centre = pixel_index.astype(jnp.float32) + 0.5
    centres = corner.astype(jnp.float32) + foot * offset
    scaled = (pixel_centre - centres[..., None]) / radius[..., None]
    bump_shape = jnp.maximum(1.0 - scaled * scaled, 0.0)
    inside = (pixel_index >= corner[..., None]) & (pixel_index < corner[..., None] + foot)
    return jnp.where(inside, bump_shape * bump_shape, 0.0)


def deposit(corner, offset, radius, emission, extinction, block_live, tile_side, foot):
    across = axis_weights(corner[0], offset[0], radius, tile_side, foot)
    down_weights = axis_weights(corner[1], offset[1], radius, tile_side, foot)
    fields = jnp.concatenate([emission, extinction[None]], 0) * block_live[None, :, None]
    spread = fields[..., None] * across[None]
    deposit_out = jnp.einsum('gpy,cgpx->gycx', down_weights, spread, precision=lax.Precision.HIGHEST)
    return deposit_out.reshape(deposit_out.shape[0], tile_side, 4 * tile_side)


def composite(stacked, slab_rank):
    slab_num, tile_num, tile_side, row_width = stacked.shape
    pieces = stacked.reshape(slab_num, tile_num, tile_side, 4, row_width // 4)
    glow_part = pieces[:, :, :, :3, :]
    optical = pieces[:, :, :, 3:, :]
    before = (slab_rank[None, :] < slab_rank[:, None]).astype(jnp.float32)
    prior_depth = jnp.einsum('jk,ktyax->jtyax', before, optical, precision=lax.Precision.HIGHEST)
    lighting = jnp.sum(jnp.exp(-prior_depth) * glow_part * jnp.exp(-0.5 * optical), axis=0)
    coverage = 1.0 - jnp.exp(-jnp.sum(optical, axis=0))
    return jnp.concatenate([lighting, coverage], axis=2).reshape(tile_num, tile_side, row_width)


def reference(block_tile, block_count, slab_rank, corner, offset, radius, emission, extinction):
    group_size = min(256, BLK_DEV)
    rounds = BLK_DEV // group_size
    tile_ids = block_tile.reshape(N_DEPTH, N_SCREEN, rounds, group_size)
    corners = jnp.moveaxis(corner.reshape(2, N_DEPTH, N_SCREEN, rounds, group_size, PB), 0, 3)
    offsets = jnp.moveaxis(offset.reshape(2, N_DEPTH, N_SCREEN, rounds, group_size, PB), 0, 3)
    radii = radius.reshape(N_DEPTH, N_SCREEN, rounds, group_size, PB)
    glows = jnp.moveaxis(emission.reshape(3, N_DEPTH, N_SCREEN, rounds, group_size, PB), 0, 3)
    rates = extinction.reshape(N_DEPTH, N_SCREEN, rounds, group_size, PB)

    def one_device(running, device_inputs):
        ids_dev, live_count, corner_dev, offset_dev, radius_dev, glow_dev, rate_dev = device_inputs
        slot_live = (jnp.arange(BLK_DEV, dtype=jnp.int32) < live_count).astype(jnp.float32)
        slot_live = slot_live.reshape(rounds, group_size)

        def one_round(tile_sums, round_inputs):
            ids_now, live_now, corner_now, offset_now, radius_now, glow_now, rate_now = round_inputs
            deposit_out = deposit(corner_now, offset_now, radius_now, glow_now, rate_now, live_now, TS, FOOT)
            return tile_sums.at[ids_now].add(deposit_out), None

        tile_sums, unused = lax.scan(one_round, jnp.zeros((TILES, TS, 4 * TS), jnp.float32),
                                     (ids_dev, slot_live, corner_dev, offset_dev, radius_dev, glow_dev, rate_dev))
        return running + tile_sums, None

    def one_slab(slab_inputs):
        running, unused = lax.scan(one_device, jnp.zeros((TILES, TS, 4 * TS), jnp.float32), slab_inputs)
        return running

    slab_stack = lax.map(one_slab, (tile_ids, block_count, corners, offsets, radii, glows, rates))
    return composite(slab_stack, slab_rank)
```

```python
import functools

import jax
import jax.numpy as jnp
from jax import lax
from jax.experimental import pallas as pl
from jax.experimental.pallas import tpu as pltpu
from jax.sharding import PartitionSpec as P

TS = 32
FOOT = 16
TILE_DEV = 4
CHUNK = 256
UNROLL = 128
SPREAD = 0.125


def deposit_kernel(chunk, unroll, count_ref, tile_ref, corner_ref, offset_ref, radius_ref,
                   emission_ref, extinction_ref, sums_ref, square_ref, shift_ref, field_ref):
    step = pl.program_id(0)
    lanes = radius_ref.shape[-1]

    @pl.when(step == 0)
    def _():
        sums_ref[...] = jnp.zeros_like(sums_ref)

    base = step * chunk
    live = jnp.clip(count_ref[0, 0] - base, 0, chunk)

    @pl.when(live > 0)
    def _():
        lane = lax.broadcasted_iota(jnp.int32, (1, lanes), 1).astype(jnp.float32)
        stretch = jnp.exp2(lane * (SPREAD / (4 * lanes)))
        area = stretch * stretch
        undo = 1.0 / (area * area)
        radius = radius_ref[0]
        square = radius * radius
        square_ref[0] = square
        square_ref[1] = square * area
        inverse = 1.0 / square
        inverse = inverse * inverse
        inverse = inverse * inverse * undo
        shift_ref[0] = 0.5 - (corner_ref[0, 0].astype(jnp.float32) + FOOT * offset_ref[0, 0])
        shift_ref[1] = (0.5 - (corner_ref[1, 0].astype(jnp.float32) + FOOT * offset_ref[1, 0])) * stretch
        alive = lax.broadcasted_iota(jnp.int32, (chunk, lanes), 0) < live
        inverse = jnp.where(alive, inverse, 0.0)
        for channel in range(3):
            field_ref[channel] = emission_ref[channel, 0] * inverse
        field_ref[3] = extinction_ref[0] * inverse

        pixel = lax.broadcasted_iota(jnp.int32, (FOOT, lanes), 0)
        near_x = pixel.astype(jnp.float32)
        far_x = near_x + FOOT
        pixel_near = (near_x, near_x * stretch)
        pixel_far = (far_x, far_x * stretch)
        nothing = jnp.zeros((FOOT, lanes), jnp.bfloat16)
        blank = jnp.zeros((2 * FOOT, lanes), jnp.bfloat16)

        def weights(axis, row):
            near = corner_ref[axis, 0, pl.ds(row, 1), :] <= pixel
            away = jnp.where(near, pixel_near[axis], pixel_far[axis]) + shift_ref[axis, pl.ds(row, 1), :]
            bump = jnp.maximum(square_ref[axis, pl.ds(row, 1), :] - away * away, 0.0)
            return near, bump * bump

        def place(near, value):
            value = value.astype(jnp.bfloat16)
            return [jnp.where(near, value, nothing), jnp.where(near, nothing, value)]

        def block(row):
            near, across = weights(0, row)
            spread = []
            for channel in range(4):
                spread += place(near, across * field_ref[channel, pl.ds(row, 1), :])
            near, down = weights(1, row)
            return jnp.concatenate(place(near, down), 0), jnp.concatenate(spread, 0)

        def group(index, carry):
            first = pl.multiple_of(index * unroll, unroll)
            products = []
            for k in range(0, unroll, 4):
                parts = [block(first + k + j) for j in range(4)]
                down = [p[0] for p in parts]
                flip = [p[1].T for p in parts]
                left = jnp.concatenate([
                    jnp.concatenate([down[0], blank], 1), jnp.concatenate([down[1], blank], 1),
                    jnp.concatenate([blank, down[2]], 1), jnp.concatenate([blank, down[3]], 1)], 0)
                right = jnp.concatenate([jnp.concatenate(flip[:2], 1), jnp.concatenate(flip[2:], 1)], 0)
                product = lax.dot_general(
                    left, right, (((1,), (0,)), ((), ())), preferred_element_type=jnp.float32)
                products += [product[:TS, :lanes], product[TS:2 * TS, lanes:],
                             product[2 * TS:3 * TS, :lanes], product[3 * TS:, lanes:]]
            for k in range(unroll):
                tile = tile_ref[0, base + first + k]
                sums_ref[tile] += products[k]
            return carry

        lax.fori_loop(0, (live + unroll - 1) // unroll, group, 0)


def deposit(block_count, block_tile, corner, offset, radius, emission, extinction, tiles_all):
    slots, lanes = radius.shape[1:]
    chunk = min(CHUNK, slots)
    unroll = min(UNROLL, chunk)

    def at(step, count_ref):
        return jnp.minimum(step, (count_ref[0, 0] - 1) // chunk)

    def wide(step, count_ref, tile_ref):
        return (0, 0, at(step, count_ref), 0)

    def narrow(step, count_ref, tile_ref):
        return (0, at(step, count_ref), 0)

    return pl.pallas_call(
        functools.partial(deposit_kernel, chunk, unroll),
        grid_spec=pltpu.PrefetchScalarGridSpec(
            num_scalar_prefetch=2,
            grid=(slots // chunk,),
            in_specs=[
                pl.BlockSpec((2, 1, chunk, lanes), wide),
                pl.BlockSpec((2, 1, chunk, lanes), wide),
                pl.BlockSpec((1, chunk, lanes), narrow),
                pl.BlockSpec((3, 1, chunk, lanes), wide),
                pl.BlockSpec((1, chunk, lanes), narrow),
            ],
            out_specs=pl.BlockSpec((tiles_all, TS, 4 * TS), lambda *_: (0, 0, 0)),
            scratch_shapes=[
                pltpu.VMEM((2, chunk, lanes), jnp.float32),
                pltpu.VMEM((2, chunk, lanes), jnp.float32),
                pltpu.VMEM((4, chunk, lanes), jnp.float32),
            ],
        ),
        out_shape=jax.ShapeDtypeStruct((tiles_all, TS, 4 * TS), jnp.float32),
        compiler_params=pltpu.CompilerParams(dimension_semantics=("arbitrary",)),
        name="deposit",
    )(block_count, block_tile, corner, offset, radius, emission, extinction)


def greet(peers):
    barrier = pltpu.get_barrier_semaphore()
    for peer in peers:
        pl.semaphore_signal(barrier, inc=1, device_id=peer, device_id_type=pl.DeviceIdType.MESH)
    pl.semaphore_wait(barrier, len(peers))


def reduce_kernel(partial_ref, slab_ref, mine_ref, held_ref, own_sem, send_sem, recv_sem):
    depth_size, screen_size = partial_ref.shape[:2]
    me = lax.axis_index("screen")
    own = pltpu.make_async_copy(partial_ref, mine_ref, own_sem)
    own.start()
    barrier = pltpu.get_barrier_semaphore()
    for step, present in ((1, me < screen_size - 1), (-1, me > 0)):
        @pl.when(present)
        def _(step=step):
            pl.semaphore_signal(barrier, inc=1, device_id={"screen": me + step},
                                device_id_type=pl.DeviceIdType.MESH)
    pl.semaphore_wait(barrier, jnp.where(me > 0, 1, 0) + jnp.where(me < screen_size - 1, 1, 0))

    def piece(side, owner, d, source):
        return pltpu.make_async_remote_copy(
            src_ref=source,
            dst_ref=held_ref.at[side, owner, d],
            send_sem=send_sem.at[side, owner, d],
            recv_sem=recv_sem.at[side, owner, d],
            device_id={"screen": me + 1 - 2 * side},
            device_id_type=pl.DeviceIdType.MESH,
        )

    def passes(side, owner):
        return (owner - me) * (1 - 2 * side) > 0

    def first(side):
        return me == side * (screen_size - 1)

    def owner_of(side, near):
        return near if side else screen_size - 1 - near

    for near in range(screen_size - 1):
        for side in range(2):
            @pl.when(first(side))
            def _(side=side, owner=owner_of(side, near)):
                def launch(d, carry):
                    piece(side, owner, d, partial_ref.at[d, owner]).start()
                    return carry

                lax.fori_loop(0, depth_size, launch, 0)
    own.wait()

    lead = jnp.where(me < screen_size // 2, 0, 1)
    for near in range(screen_size - 1):
        for side in (lead, 1 - lead):
            owner = jnp.where(side == 1, near, screen_size - 1 - near)

            @pl.when(jnp.logical_and(passes(side, owner), me != side * (screen_size - 1)))
            def _(side=side, owner=owner):
                def relay(d, carry):
                    piece(side, owner, d, held_ref.at[side, owner, d]).wait_recv()
                    held_ref[side, owner, d] += mine_ref[d, owner]
                    piece(side, owner, d, held_ref.at[side, owner, d]).start()
                    return carry

                lax.fori_loop(0, depth_size, relay, 0)

    def collect(d, carry):
        slab_ref[d] = mine_ref[d, me]
        for side in range(2):
            @pl.when(jnp.logical_not(first(side)))
            def _(side=side):
                piece(side, me, d, held_ref.at[side, me, d]).wait_recv()
                slab_ref[d] += held_ref[side, me, d]
        return carry

    lax.fori_loop(0, depth_size, collect, 0)

    def finish(d, carry):
        for side in range(2):
            for owner in range(screen_size):
                @pl.when(passes(side, owner))
                def _(side=side, owner=owner):
                    piece(side, owner, d, held_ref.at[side, owner, d]).wait_send()
        return carry

    lax.fori_loop(0, depth_size, finish, 0)


def reduce_screen(partial_value):
    depth_size, screen_size, rows, lanes = partial_value.shape
    return pl.pallas_call(
        reduce_kernel,
        in_specs=[pl.BlockSpec(memory_space=pl.ANY)],
        out_specs=pl.BlockSpec(memory_space=pltpu.VMEM),
        out_shape=jax.ShapeDtypeStruct((depth_size, rows, lanes), jnp.float32),
        scratch_shapes=[
            pltpu.VMEM(partial_value.shape, jnp.float32),
            pltpu.VMEM((2, screen_size, depth_size, rows, lanes), jnp.float32),
            pltpu.SemaphoreType.DMA,
            pltpu.SemaphoreType.DMA((2, screen_size, depth_size)),
            pltpu.SemaphoreType.DMA((2, screen_size, depth_size)),
        ],
        compiler_params=pltpu.CompilerParams(collective_id=0, has_side_effects=True),
        name="reduce",
    )(partial_value)


def composite_kernel(rank_ref, slab_ref, image_ref, stack_ref, own_sem, send_sem, recv_sem):
    depth_size = slab_ref.shape[0]
    me = lax.axis_index("depth")
    others = [lax.rem(me + hop, depth_size) for hop in range(1, depth_size)]
    own = pltpu.make_async_copy(slab_ref.at[me], stack_ref.at[me], own_sem)
    own.start()
    greet([{"depth": other} for other in others])

    def piece(hop):
        return pltpu.make_async_remote_copy(
            src_ref=slab_ref.at[others[hop]],
            dst_ref=stack_ref.at[me],
            send_sem=send_sem.at[hop],
            recv_sem=recv_sem.at[hop],
            device_id={"depth": others[hop]},
            device_id_type=pl.DeviceIdType.MESH,
        )

    for hop in range(depth_size - 1):
        piece(hop).start()
    own.wait()
    for hop in range(depth_size - 1):
        piece(hop).wait_recv()

    lanes = slab_ref.shape[-1]
    quarter = lanes // 4
    before = [[jnp.where(rank_ref[k] < rank_ref[j], 1.0, 0.0) for k in range(depth_size)]
              for j in range(depth_size)]
    rows_at_once = 16
    lane = lax.broadcasted_iota(jnp.int32, (rows_at_once, lanes), 1)
    optical_lane = lane >= 3 * quarter

    def rows_of(index, carry):
        rows = pl.ds(pl.multiple_of(index * rows_at_once, rows_at_once), rows_at_once)
        depths = []
        for k in range(depth_size):
            optical = jnp.where(optical_lane, stack_ref[k, rows], 0.0)
            optical = optical + pltpu.roll(optical, 2 * quarter, 1)
            depths.append(optical + pltpu.roll(optical, quarter, 1))
        lighting = jnp.zeros((rows_at_once, lanes), jnp.float32)
        for j in range(depth_size):
            reach = 0.5 * depths[j]
            for k in range(depth_size):
                if k != j:
                    reach = reach + before[j][k] * depths[k]
            lighting = lighting + jnp.exp(-reach) * stack_ref[j, rows]
        whole = depths[0]
        for k in range(1, depth_size):
            whole = whole + depths[k]
        image_ref[rows] = jnp.where(optical_lane, 1.0 - jnp.exp(-whole), lighting)
        return carry

    lax.fori_loop(0, slab_ref.shape[1] // rows_at_once, rows_of, 0)
    for hop in range(depth_size - 1):
        piece(hop).wait_send()


def composite_depth(slab, slab_rank):
    depth_size, rows, lanes = slab.shape
    hops = max(depth_size - 1, 1)
    return pl.pallas_call(
        composite_kernel,
        in_specs=[pl.BlockSpec(memory_space=pltpu.SMEM), pl.BlockSpec(memory_space=pltpu.VMEM)],
        out_specs=pl.BlockSpec(memory_space=pltpu.VMEM),
        out_shape=jax.ShapeDtypeStruct((rows, lanes), jnp.float32),
        scratch_shapes=[
            pltpu.VMEM((depth_size, rows, lanes), jnp.float32),
            pltpu.SemaphoreType.DMA,
            pltpu.SemaphoreType.DMA((hops,)),
            pltpu.SemaphoreType.DMA((hops,)),
        ],
        compiler_params=pltpu.CompilerParams(collective_id=1, has_side_effects=True),
        name="composite",
    )(slab_rank, slab)


def shards(block_tile, block_count, slab_rank, corner, offset, radius, emission, extinction):
    depth_size = lax.axis_size("depth")
    screen_size = lax.axis_size("screen")
    tiles_all = TILE_DEV * depth_size * screen_size
    partial_value = deposit(
        block_count, block_tile, corner, offset, radius, emission, extinction, tiles_all)
    slab = reduce_screen(partial_value.reshape(depth_size, screen_size, TILE_DEV * TS, 4 * TS))
    return composite_depth(slab, slab_rank).reshape(TILE_DEV, TS, 4 * TS)


def solution(mesh):
    placed = (
        P("depth", "screen"),
        P("depth", "screen"),
        P(),
        P(None, "depth", "screen", None),
        P(None, "depth", "screen", None),
        P("depth", "screen", None),
        P(None, "depth", "screen", None),
        P("depth", "screen", None),
    )
    return jax.shard_map(
        shards,
        mesh=mesh,
        in_specs=placed,
        out_specs=P(("depth", "screen"), None, None),
        check_vma=False,
    )
```

```python
import functools

import jax
import jax.numpy as jnp
from jax import lax
from jax.experimental import pallas as pl
from jax.experimental.pallas import tpu as pltpu
from jax.sharding import PartitionSpec as P

TS = 32
FOOT = 16
TILE_DEV = 4
CHUNK = 256
UNROLL = 128
SPREAD = 0.125
CUTS = 2
LAG = 3


def deposit_kernel(chunk, unroll, count_ref, tile_ref, corner_ref, offset_ref, radius_ref,
                   emission_ref, extinction_ref, sums_ref, square_ref, shift_ref, field_ref):
    step = pl.program_id(0)
    lanes = radius_ref.shape[-1]

    @pl.when(step == 0)
    def _():
        sums_ref[...] = jnp.zeros_like(sums_ref)

    base = step * chunk
    live = jnp.clip(count_ref[0, 0] - base, 0, chunk)

    @pl.when(live > 0)
    def _():
        lane = lax.broadcasted_iota(jnp.int32, (1, lanes), 1).astype(jnp.float32)
        stretch = jnp.exp2(lane * (SPREAD / (4 * lanes)))
        area = stretch * stretch
        undo = 1.0 / (area * area)
        radius = radius_ref[0]
        square = radius * radius
        square_ref[0] = square
        square_ref[1] = square * area
        inverse = 1.0 / square
        inverse = inverse * inverse
        inverse = inverse * inverse * undo
        shift_ref[0] = 0.5 - (corner_ref[0, 0].astype(jnp.float32) + FOOT * offset_ref[0, 0])
        shift_ref[1] = (0.5 - (corner_ref[1, 0].astype(jnp.float32) + FOOT * offset_ref[1, 0])) * stretch
        alive = lax.broadcasted_iota(jnp.int32, (chunk, lanes), 0) < live
        inverse = jnp.where(alive, inverse, 0.0)
        for channel in range(3):
            field_ref[channel] = emission_ref[channel, 0] * inverse
        field_ref[3] = extinction_ref[0] * inverse

        pixel = lax.broadcasted_iota(jnp.int32, (FOOT, lanes), 0)
        near_x = pixel.astype(jnp.float32)
        far_x = near_x + FOOT
        pixel_near = (near_x, near_x * stretch)
        pixel_far = (far_x, far_x * stretch)
        nothing = jnp.zeros((FOOT, lanes), jnp.bfloat16)
        blank = jnp.zeros((2 * FOOT, lanes), jnp.bfloat16)

        def weights(axis, row):
            near = corner_ref[axis, 0, pl.ds(row, 1), :] <= pixel
            away = jnp.where(near, pixel_near[axis], pixel_far[axis]) + shift_ref[axis, pl.ds(row, 1), :]
            bump = jnp.maximum(square_ref[axis, pl.ds(row, 1), :] - away * away, 0.0)
            return near, bump * bump

        def place(near, value):
            value = value.astype(jnp.bfloat16)
            return [jnp.where(near, value, nothing), jnp.where(near, nothing, value)]

        def block(row):
            near, across = weights(0, row)
            spread = []
            for channel in range(4):
                spread += place(near, across * field_ref[channel, pl.ds(row, 1), :])
            near, down = weights(1, row)
            return jnp.concatenate(place(near, down), 0), jnp.concatenate(spread, 0)

        def group(index, carry):
            first = pl.multiple_of(index * unroll, unroll)
            products = []
            for k in range(0, unroll, 4):
                parts = [block(first + k + j) for j in range(4)]
                down = [p[0] for p in parts]
                flip = [p[1].T for p in parts]
                left = jnp.concatenate([
                    jnp.concatenate([down[0], blank], 1), jnp.concatenate([down[1], blank], 1),
                    jnp.concatenate([blank, down[2]], 1), jnp.concatenate([blank, down[3]], 1)], 0)
                right = jnp.concatenate([jnp.concatenate(flip[:2], 1), jnp.concatenate(flip[2:], 1)], 0)
                product = lax.dot_general(
                    left, right, (((1,), (0,)), ((), ())), preferred_element_type=jnp.float32)
                products += [product[:TS, :lanes], product[TS:2 * TS, lanes:],
                             product[2 * TS:3 * TS, :lanes], product[3 * TS:, lanes:]]
            for k in range(unroll):
                tile = tile_ref[0, base + first + k]
                sums_ref[tile] += products[k]
            return carry

        lax.fori_loop(0, (live + unroll - 1) // unroll, group, 0)


def deposit(block_count, block_tile, corner, offset, radius, emission, extinction, tiles_all):
    slots, lanes = radius.shape[1:]
    chunk = min(CHUNK, slots)
    unroll = min(UNROLL, chunk)

    def at(step, count_ref):
        return jnp.minimum(step, (count_ref[0, 0] - 1) // chunk)

    def wide(step, count_ref, tile_ref):
        return (0, 0, at(step, count_ref), 0)

    def narrow(step, count_ref, tile_ref):
        return (0, at(step, count_ref), 0)

    return pl.pallas_call(
        functools.partial(deposit_kernel, chunk, unroll),
        grid_spec=pltpu.PrefetchScalarGridSpec(
            num_scalar_prefetch=2,
            grid=(slots // chunk,),
            in_specs=[
                pl.BlockSpec((2, 1, chunk, lanes), wide),
                pl.BlockSpec((2, 1, chunk, lanes), wide),
                pl.BlockSpec((1, chunk, lanes), narrow),
                pl.BlockSpec((3, 1, chunk, lanes), wide),
                pl.BlockSpec((1, chunk, lanes), narrow),
            ],
            out_specs=pl.BlockSpec((tiles_all, TS, 4 * TS), lambda *_: (0, 0, 0)),
            scratch_shapes=[
                pltpu.VMEM((2, chunk, lanes), jnp.float32),
                pltpu.VMEM((2, chunk, lanes), jnp.float32),
                pltpu.VMEM((4, chunk, lanes), jnp.float32),
            ],
        ),
        out_shape=jax.ShapeDtypeStruct((tiles_all, TS, 4 * TS), jnp.float32),
        compiler_params=pltpu.CompilerParams(dimension_semantics=("arbitrary",)),
        name="deposit",
    )(block_count, block_tile, corner, offset, radius, emission, extinction)


def signal(barrier, device):
    pl.semaphore_signal(barrier, inc=1, device_id=device, device_id_type=pl.DeviceIdType.MESH)


def exchange_kernel(rank_ref, partial_ref, image_ref, mine_ref, held_ref, stack_ref, ready_ref, landed_ref,
                    own_sem, send_sem, recv_sem, out_sem, in_sem, image_send_sem, image_recv_sem):
    depth_size, screen_size, rows, lanes = partial_ref.shape
    half = screen_size // 2
    part = rows // CUTS
    pieces = half * depth_size * CUTS
    edge = (screen_size - 1, 0)
    me = lax.axis_index("screen")
    slab = lax.axis_index("depth")
    own = pltpu.make_async_copy(partial_ref, mine_ref, own_sem)
    own.start()

    at_edge = jnp.logical_or(me == 0, me == screen_size - 1)
    far = jnp.logical_and(jnp.logical_not(at_edge), jnp.where(me < half, me > 1, me < screen_size - 2))
    barrier = pltpu.get_barrier_semaphore()
    counts = []

    def greet(present, device):
        counts.append(jnp.where(present, 1, 0))

        @pl.when(present)
        def _():
            signal(barrier, device)

    greet(me > 0, {"screen": me - 1})
    greet(me < screen_size - 1, {"screen": me + 1})
    for hop in range(1, depth_size):
        greet(at_edge, {"depth": lax.rem(slab + hop, depth_size)})
    greet(far, {"screen": jnp.where(me < half, 0, screen_size - 1)})
    for other in range(2, half):
        greet(me == 0, {"screen": other})
        greet(me == screen_size - 1, {"screen": screen_size - 1 - other})
    total = counts[0]
    for count in counts[1:]:
        total = total + count
    pl.semaphore_wait(barrier, total)

    def place(side, j):
        group = j // (depth_size * CUTS)
        inside = lax.rem(j, depth_size * CUTS)
        target = lax.rem(slab + 1 + inside // CUTS, depth_size)
        owner = half - 1 - group if side else half + group
        return group, target, owner, lax.rem(inside, CUTS)

    def rows_of(cut):
        return pl.ds(pl.multiple_of(cut * part, part), part)

    def hop(side, j, source):
        return pltpu.make_async_remote_copy(
            src_ref=source, dst_ref=held_ref.at[side, j],
            send_sem=send_sem.at[side, j], recv_sem=recv_sem.at[side, j],
            device_id={"screen": me + 1 - 2 * side}, device_id_type=pl.DeviceIdType.MESH)

    def across_of(side, j, group, target, cut):
        return pltpu.make_async_remote_copy(
            src_ref=held_ref.at[side, j], dst_ref=stack_ref.at[group, slab, rows_of(cut)],
            send_sem=out_sem.at[j], recv_sem=in_sem.at[group, slab, cut],
            device_id={"depth": target}, device_id_type=pl.DeviceIdType.MESH)

    def arrival(group, source, cut):
        return pltpu.make_async_remote_copy(
            src_ref=held_ref.at[0, 0], dst_ref=stack_ref.at[group, source, rows_of(cut)],
            send_sem=out_sem.at[0], recv_sem=in_sem.at[group, source, cut],
            device_id={"depth": source}, device_id_type=pl.DeviceIdType.MESH)

    def handed(group, owner):
        return pltpu.make_async_remote_copy(
            src_ref=ready_ref.at[group], dst_ref=landed_ref,
            send_sem=image_send_sem.at[group], recv_sem=image_recv_sem,
            device_id={"screen": owner}, device_id_type=pl.DeviceIdType.MESH)

    for side in range(2):
        @pl.when(me == side * (screen_size - 1))
        def _(side=side):
            def launch(j, carry):
                group, target, owner, cut = place(side, j)
                hop(side, j, partial_ref.at[target, owner, rows_of(cut)]).start()
                return carry

            lax.fori_loop(0, pieces, launch, 0)
    own.wait()

    @pl.when(jnp.logical_not(at_edge))
    def _():
        late = [LAG * jnp.maximum(2 * me - (screen_size - 1), 0),
                LAG * jnp.maximum((screen_size - 1) - 2 * me, 0)]

        def relay(i, carry):
            for side in range(2):
                j = i - late[side]

                @pl.when(jnp.logical_and(j >= 0, j < pieces))
                def _(side=side, j=j):
                    group, target, owner, cut = place(side, j)
                    move = hop(side, j, held_ref.at[side, j])
                    move.wait_recv()
                    held_ref[side, j] += mine_ref[target, owner, rows_of(cut)]
                    move.start()
            return carry

        lax.fori_loop(0, pieces + LAG * (screen_size - 1), relay, 0)

    quarter = lanes // 4
    at_once = 16

    def composite(group, out_ref):
        before = [[jnp.where(rank_ref[k] < rank_ref[j], 1.0, 0.0) for k in range(depth_size)]
                  for j in range(depth_size)]
        lane = lax.broadcasted_iota(jnp.int32, (at_once, lanes), 1)
        optical_lane = lane >= 3 * quarter

        def step(index, carry):
            now = pl.ds(pl.multiple_of(index * at_once, at_once), at_once)
            depths = []
            for k in range(depth_size):
                optical = jnp.where(optical_lane, stack_ref[group, k, now], 0.0)
                optical = optical + pltpu.roll(optical, 2 * quarter, 1)
                depths.append(optical + pltpu.roll(optical, quarter, 1))
            lighting = jnp.zeros((at_once, lanes), jnp.float32)
            for j in range(depth_size):
                reach = 0.5 * depths[j]
                for k in range(depth_size):
                    if k != j:
                        reach = reach + before[j][k] * depths[k]
                lighting = lighting + jnp.exp(-reach) * stack_ref[group, j, now]
            whole = depths[0]
            for k in range(1, depth_size):
                whole = whole + depths[k]
            out_ref[now] = jnp.where(optical_lane, 1.0 - jnp.exp(-whole), lighting)
            return carry

        lax.fori_loop(0, rows // at_once, step, 0)

    def gather(group):
        def one(i, carry):
            source = lax.rem(slab + 1 + i // CUTS, depth_size)
            arrival(group, source, lax.rem(i, CUTS)).wait_recv()
            return carry

        lax.fori_loop(0, (depth_size - 1) * CUTS, one, 0)

    for side in range(2):
        @pl.when(me == edge[side])
        def _(side=side):
            def collect(j, carry):
                group, target, owner, cut = place(side, j)
                hop(side, j, held_ref.at[side, j]).wait_recv()

                @pl.when(target != slab)
                def _():
                    held_ref[side, j] += mine_ref[target, owner, rows_of(cut)]
                    across_of(side, j, group, target, cut).start()

                @pl.when(target == slab)
                def _():
                    stack_ref[group, slab, rows_of(cut)] = (
                        held_ref[side, j] + mine_ref[target, owner, rows_of(cut)])
                return carry

            share = depth_size * CUTS
            for group in range(half):
                lax.fori_loop(group * share, (group + 1) * share, collect, 0)
                if group > 0:
                    gather(group - 1)
                    composite(group - 1, ready_ref.at[group - 1])
                    handed(group - 1, half - group if side else half + group - 1).start()
            gather(half - 1)
            composite(half - 1, image_ref)

            def sent(j, carry):
                group, target, owner, cut = place(side, j)

                @pl.when(target != slab)
                def _():
                    across_of(side, j, group, target, cut).wait_send()
                return carry

            lax.fori_loop(0, pieces, sent, 0)
            for group in range(half - 1):
                handed(group, half - 1 - group if side else half + group).wait_send()

    @pl.when(jnp.logical_not(at_edge))
    def _():
        handed(0, me).wait_recv()
        image_ref[...] = landed_ref[...]

    for side in range(2):
        @pl.when(me != edge[side])
        def _(side=side):
            def gone(j, carry):
                hop(side, j, held_ref.at[side, j]).wait_send()
                return carry

            lax.fori_loop(0, pieces, gone, 0)


def exchange(partial_value, slab_rank):
    depth_size, screen_size, rows, lanes = partial_value.shape
    half = screen_size // 2
    pieces = half * depth_size * CUTS
    return pl.pallas_call(
        exchange_kernel,
        in_specs=[pl.BlockSpec(memory_space=pltpu.SMEM), pl.BlockSpec(memory_space=pl.ANY)],
        out_specs=pl.BlockSpec(memory_space=pltpu.VMEM),
        out_shape=jax.ShapeDtypeStruct((rows, lanes), jnp.float32),
        scratch_shapes=[
            pltpu.VMEM(partial_value.shape, jnp.float32),
            pltpu.VMEM((2, pieces, rows // CUTS, lanes), jnp.float32),
            pltpu.VMEM((half, depth_size, rows, lanes), jnp.float32),
            pltpu.VMEM((max(half - 1, 1), rows, lanes), jnp.float32),
            pltpu.VMEM((rows, lanes), jnp.float32),
            pltpu.SemaphoreType.DMA,
            pltpu.SemaphoreType.DMA((2, pieces)),
            pltpu.SemaphoreType.DMA((2, pieces)),
            pltpu.SemaphoreType.DMA((pieces,)),
            pltpu.SemaphoreType.DMA((half, depth_size, CUTS)),
            pltpu.SemaphoreType.DMA((max(half - 1, 1),)),
            pltpu.SemaphoreType.DMA,
        ],
        compiler_params=pltpu.CompilerParams(collective_id=0, has_side_effects=True),
        name="exchange",
    )(slab_rank, partial_value)


def shards(block_tile, block_count, slab_rank, corner, offset, radius, emission, extinction):
    depth_size = lax.axis_size("depth")
    screen_size = lax.axis_size("screen")
    tiles_all = TILE_DEV * depth_size * screen_size
    partial_value = deposit(
        block_count, block_tile, corner, offset, radius, emission, extinction, tiles_all)
    gathered = partial_value.reshape(depth_size, screen_size, TILE_DEV * TS, 4 * TS)
    return exchange(gathered, slab_rank).reshape(TILE_DEV, TS, 4 * TS)


def solution(mesh):
    placed = (
        P("depth", "screen"),
        P("depth", "screen"),
        P(),
        P(None, "depth", "screen", None),
        P(None, "depth", "screen", None),
        P("depth", "screen", None),
        P(None, "depth", "screen", None),
        P("depth", "screen", None),
    )
    return jax.shard_map(
        shards,
        mesh=mesh,
        in_specs=placed,
        out_specs=P(("depth", "screen"), None, None),
        check_vma=False,
    )
```

```python
import functools

import jax
import jax.numpy as jnp
from jax import lax
from jax.experimental import pallas as pl
from jax.experimental.pallas import tpu as pltpu
from jax.sharding import PartitionSpec as P

TS = 32
FOOT = 16
TILE_DEV = 4
CHUNK = 256
UNROLL = 256
SPREAD = 0.125
CYCLE = 4
FLIPPED = 3
CUTS = 2
LAG = 4


def deposit_kernel(chunk, unroll, count_ref, tile_ref, corner_ref, offset_ref, radius_ref,
                   emission_ref, extinction_ref, sums_ref, square_ref, shift_ref, field_ref):
    step = pl.program_id(0)
    lanes = radius_ref.shape[-1]

    @pl.when(step == 0)
    def _():
        sums_ref[...] = jnp.zeros_like(sums_ref)

    base = step * chunk
    live = jnp.clip(count_ref[0, 0] - base, 0, chunk)

    @pl.when(live > 0)
    def _():
        lane = lax.broadcasted_iota(jnp.int32, (1, lanes), 1).astype(jnp.float32)
        stretch = jnp.exp2(lane * (SPREAD / (4 * lanes)))
        area = stretch * stretch
        undo = 1.0 / (area * area)
        radius = radius_ref[0]
        square = radius * radius
        square_ref[0] = square
        square_ref[1] = square * area
        inverse = 1.0 / square
        inverse = inverse * inverse
        inverse = inverse * inverse * undo
        shift_ref[0] = 0.5 - (corner_ref[0, 0].astype(jnp.float32) + FOOT * offset_ref[0, 0])
        shift_ref[1] = (0.5 - (corner_ref[1, 0].astype(jnp.float32) + FOOT * offset_ref[1, 0])) * stretch
        alive = lax.broadcasted_iota(jnp.int32, (chunk, lanes), 0) < live
        inverse = jnp.where(alive, inverse, 0.0)
        for channel in range(3):
            field_ref[channel] = emission_ref[channel, 0] * inverse
        field_ref[3] = extinction_ref[0] * inverse

        pixel = lax.broadcasted_iota(jnp.int32, (FOOT, lanes), 0)
        near_x = pixel.astype(jnp.float32)
        far_x = near_x + FOOT
        pixel_near = (near_x, near_x * stretch)
        pixel_far = (far_x, far_x * stretch)
        nothing = jnp.zeros((FOOT, lanes), jnp.bfloat16)
        blank = jnp.zeros((2 * FOOT, lanes), jnp.bfloat16)

        def weights(axis, row):
            near = corner_ref[axis, 0, pl.ds(row, 1), :] <= pixel
            away = jnp.where(near, pixel_near[axis], pixel_far[axis]) + shift_ref[axis, pl.ds(row, 1), :]
            bump = jnp.maximum(square_ref[axis, pl.ds(row, 1), :] - away * away, 0.0)
            return near, bump * bump

        def place(near, value):
            value = value.astype(jnp.bfloat16)
            return [jnp.where(near, value, nothing), value]

        def block(row):
            near, across = weights(0, row)
            spread = []
            for channel in range(4):
                spread += place(near, across * field_ref[channel, pl.ds(row, 1), :])
            near, down = weights(1, row)
            return jnp.concatenate(place(near, down), 0), jnp.concatenate(spread, 0)

        def group(index, carry):
            first = pl.multiple_of(index * unroll, unroll)
            products = []
            for k in range(0, unroll, 4):
                parts = [block(first + k + j) for j in range(4)]
                down = [p[0] for p in parts]
                if k // 4 % CYCLE < FLIPPED:
                    side = [p[1].T for p in parts]
                    left = jnp.concatenate([
                        jnp.concatenate([down[0], blank], 1), jnp.concatenate([down[1], blank], 1),
                        jnp.concatenate([blank, down[2]], 1), jnp.concatenate([blank, down[3]], 1)], 0)
                    across_axis, keep = 0, (0, 1, 0, 1)
                else:
                    side = [p[1] for p in parts]
                    left = jnp.concatenate([
                        jnp.concatenate([down[0], blank], 1), jnp.concatenate([blank, down[1]], 1),
                        jnp.concatenate([down[2], blank], 1), jnp.concatenate([blank, down[3]], 1)], 0)
                    across_axis, keep = 1, (0, 0, 1, 1)
                right = jnp.concatenate([jnp.concatenate(side[:2], 1), jnp.concatenate(side[2:], 1)], 0)
                product = lax.dot_general(
                    left, right, (((1,), (across_axis,)), ((), ())), preferred_element_type=jnp.float32)
                products += [product[j * TS:(j + 1) * TS, keep[j] * lanes:(keep[j] + 1) * lanes]
                             for j in range(4)]
            for k in range(unroll):
                tile = tile_ref[0, base + first + k]
                sums_ref[tile] += products[k]
            return carry

        lax.fori_loop(0, (live + unroll - 1) // unroll, group, 0)


def deposit(block_count, block_tile, corner, offset, radius, emission, extinction, tiles_all):
    slots, lanes = radius.shape[1:]
    chunk = min(CHUNK, slots)
    unroll = min(UNROLL, chunk)

    def at(step, count_ref):
        return jnp.minimum(step, (count_ref[0, 0] - 1) // chunk)

    def wide(step, count_ref, tile_ref):
        return (0, 0, at(step, count_ref), 0)

    def narrow(step, count_ref, tile_ref):
        return (0, at(step, count_ref), 0)

    return pl.pallas_call(
        functools.partial(deposit_kernel, chunk, unroll),
        grid_spec=pltpu.PrefetchScalarGridSpec(
            num_scalar_prefetch=2,
            grid=(slots // chunk,),
            in_specs=[
                pl.BlockSpec((2, 1, chunk, lanes), wide),
                pl.BlockSpec((2, 1, chunk, lanes), wide),
                pl.BlockSpec((1, chunk, lanes), narrow),
                pl.BlockSpec((3, 1, chunk, lanes), wide),
                pl.BlockSpec((1, chunk, lanes), narrow),
            ],
            out_specs=pl.BlockSpec((tiles_all, TS, 4 * TS), lambda *_: (0, 0, 0)),
            scratch_shapes=[
                pltpu.VMEM((2, chunk, lanes), jnp.float32),
                pltpu.VMEM((2, chunk, lanes), jnp.float32),
                pltpu.VMEM((4, chunk, lanes), jnp.float32),
            ],
        ),
        out_shape=jax.ShapeDtypeStruct((tiles_all, TS, 4 * TS), jnp.float32),
        compiler_params=pltpu.CompilerParams(dimension_semantics=("arbitrary",)),
        name="deposit",
    )(block_count, block_tile, corner, offset, radius, emission, extinction)


def signal(barrier, device):
    pl.semaphore_signal(barrier, inc=1, device_id=device, device_id_type=pl.DeviceIdType.MESH)


def exchange_kernel(rank_ref, partial_ref, image_ref, mine_ref, held_ref, stack_ref, ready_ref, landed_ref,
                    own_sem, send_sem, recv_sem, out_sem, in_sem, image_send_sem, image_recv_sem):
    depth_size, screen_size, rows, lanes = partial_ref.shape
    half = screen_size // 2
    part = rows // CUTS
    pieces = half * depth_size * CUTS
    edge = (screen_size - 1, 0)
    me = lax.axis_index("screen")
    slab = lax.axis_index("depth")
    own = pltpu.make_async_copy(partial_ref, mine_ref, own_sem)
    own.start()

    at_edge = jnp.logical_or(me == 0, me == screen_size - 1)
    far = jnp.logical_and(jnp.logical_not(at_edge), jnp.where(me < half, me > 1, me < screen_size - 2))
    barrier = pltpu.get_barrier_semaphore()
    counts = []

    def greet(present, device):
        counts.append(jnp.where(present, 1, 0))

        @pl.when(present)
        def _():
            signal(barrier, device)

    greet(me > 0, {"screen": me - 1})
    greet(me < screen_size - 1, {"screen": me + 1})
    for hop in range(1, depth_size):
        greet(at_edge, {"depth": lax.rem(slab + hop, depth_size)})
    greet(far, {"screen": jnp.where(me < half, 0, screen_size - 1)})
    for other in range(2, half):
        greet(me == 0, {"screen": other})
        greet(me == screen_size - 1, {"screen": screen_size - 1 - other})
    total = counts[0]
    for count in counts[1:]:
        total = total + count
    pl.semaphore_wait(barrier, total)

    def place(side, j):
        group = j // (depth_size * CUTS)
        inside = lax.rem(j, depth_size * CUTS)
        target = lax.rem(slab + 1 + inside // CUTS, depth_size)
        owner = jnp.where(side == 1, half - 1 - group, half + group)
        return group, target, owner, lax.rem(inside, CUTS)

    def rows_of(cut):
        return pl.ds(pl.multiple_of(cut * part, part), part)

    def hop(side, j, source):
        return pltpu.make_async_remote_copy(
            src_ref=source, dst_ref=held_ref.at[side, j],
            send_sem=send_sem.at[side, j], recv_sem=recv_sem.at[side, j],
            device_id={"screen": me + 1 - 2 * side}, device_id_type=pl.DeviceIdType.MESH)

    def across_of(side, j, group, target, cut):
        return pltpu.make_async_remote_copy(
            src_ref=held_ref.at[side, j], dst_ref=stack_ref.at[group, slab, rows_of(cut)],
            send_sem=out_sem.at[j], recv_sem=in_sem.at[group, slab, cut],
            device_id={"depth": target}, device_id_type=pl.DeviceIdType.MESH)

    def arrival(group, source, cut):
        return pltpu.make_async_remote_copy(
            src_ref=held_ref.at[0, 0], dst_ref=stack_ref.at[group, source, rows_of(cut)],
            send_sem=out_sem.at[0], recv_sem=in_sem.at[group, source, cut],
            device_id={"depth": source}, device_id_type=pl.DeviceIdType.MESH)

    def handed(group, owner):
        return pltpu.make_async_remote_copy(
            src_ref=ready_ref.at[group], dst_ref=landed_ref,
            send_sem=image_send_sem.at[group], recv_sem=image_recv_sem,
            device_id={"screen": owner}, device_id_type=pl.DeviceIdType.MESH)

    for side in range(2):
        @pl.when(me == side * (screen_size - 1))
        def _(side=side):
            def launch(j, carry):
                group, target, owner, cut = place(side, j)
                hop(side, j, partial_ref.at[target, owner, rows_of(cut)]).start()
                return carry

            lax.fori_loop(0, pieces, launch, 0)
    own.wait()

    @pl.when(jnp.logical_not(at_edge))
    def _():
        lead = jnp.where(me < half, 0, 1)
        behind = LAG * jnp.abs(2 * me - (screen_size - 1))

        def forward(side, j):
            @pl.when(jnp.logical_and(j >= 0, j < pieces))
            def _():
                group, target, owner, cut = place(side, j)
                move = hop(side, j, held_ref.at[side, j])
                move.wait_recv()
                held_ref[side, j] += mine_ref[target, owner, rows_of(cut)]
                move.start()

        def relay(i, carry):
            forward(lead, i)
            forward(1 - lead, i - behind)
            return carry

        lax.fori_loop(0, pieces + LAG * (screen_size - 1), relay, 0)

    quarter = lanes // 4
    at_once = TS

    def composite(group, out_ref):
        before = [[jnp.where(rank_ref[k] < rank_ref[j], 1.0, 0.0) for k in range(depth_size)]
                  for j in range(depth_size)]
        lane = lax.broadcasted_iota(jnp.int32, (at_once, lanes), 1)
        optical_lane = lane >= 3 * quarter

        low_lane = lax.rem(lane, 2 * FOOT) < FOOT

        def whole_rows(k, index):
            near = stack_ref[group, k, pl.ds(pl.multiple_of(index * TS, TS), FOOT)]
            total = stack_ref[group, k, pl.ds(pl.multiple_of(index * TS + FOOT, FOOT), FOOT)]
            both = jnp.concatenate([near, total - near], 0)
            return both - jnp.where(low_lane, 0.0, pltpu.roll(both, FOOT, 1))

        def step(index, carry):
            now = pl.ds(pl.multiple_of(index * at_once, at_once), at_once)
            slabs = [whole_rows(k, index) for k in range(depth_size)]
            depths = []
            for k in range(depth_size):
                optical = jnp.where(optical_lane, slabs[k], 0.0)
                optical = optical + pltpu.roll(optical, 2 * quarter, 1)
                depths.append(optical + pltpu.roll(optical, quarter, 1))
            lighting = jnp.zeros((at_once, lanes), jnp.float32)
            for j in range(depth_size):
                reach = 0.5 * depths[j]
                for k in range(depth_size):
                    if k != j:
                        reach = reach + before[j][k] * depths[k]
                lighting = lighting + jnp.exp(-reach) * slabs[j]
            whole = depths[0]
            for k in range(1, depth_size):
                whole = whole + depths[k]
            out_ref[now] = jnp.where(optical_lane, 1.0 - jnp.exp(-whole), lighting)
            return carry

        lax.fori_loop(0, rows // at_once, step, 0)

    def gather(group):
        def one(i, carry):
            source = lax.rem(slab + 1 + i // CUTS, depth_size)
            arrival(group, source, lax.rem(i, CUTS)).wait_recv()
            return carry

        lax.fori_loop(0, (depth_size - 1) * CUTS, one, 0)

    for side in range(2):
        @pl.when(me == edge[side])
        def _(side=side):
            def collect(j, carry):
                group, target, owner, cut = place(side, j)
                hop(side, j, held_ref.at[side, j]).wait_recv()

                @pl.when(target != slab)
                def _():
                    held_ref[side, j] += mine_ref[target, owner, rows_of(cut)]
                    across_of(side, j, group, target, cut).start()

                @pl.when(target == slab)
                def _():
                    stack_ref[group, slab, rows_of(cut)] = (
                        held_ref[side, j] + mine_ref[target, owner, rows_of(cut)])
                return carry

            share = depth_size * CUTS
            for group in range(half):
                lax.fori_loop(group * share, (group + 1) * share, collect, 0)
                if group > 0:
                    gather(group - 1)
                    composite(group - 1, ready_ref.at[group - 1])
                    handed(group - 1, half - group if side else half + group - 1).start()
            gather(half - 1)
            composite(half - 1, image_ref)

            def sent(j, carry):
                group, target, owner, cut = place(side, j)

                @pl.when(target != slab)
                def _():
                    across_of(side, j, group, target, cut).wait_send()
                return carry

            lax.fori_loop(0, pieces, sent, 0)
            for group in range(half - 1):
                handed(group, half - 1 - group if side else half + group).wait_send()

    @pl.when(jnp.logical_not(at_edge))
    def _():
        handed(0, me).wait_recv()
        image_ref[...] = landed_ref[...]

    for side in range(2):
        @pl.when(me != edge[side])
        def _(side=side):
            def gone(j, carry):
                hop(side, j, held_ref.at[side, j]).wait_send()
                return carry

            lax.fori_loop(0, pieces, gone, 0)


def exchange(partial_value, slab_rank):
    depth_size, screen_size, rows, lanes = partial_value.shape
    half = screen_size // 2
    pieces = half * depth_size * CUTS
    return pl.pallas_call(
        exchange_kernel,
        in_specs=[pl.BlockSpec(memory_space=pltpu.SMEM), pl.BlockSpec(memory_space=pl.ANY)],
        out_specs=pl.BlockSpec(memory_space=pltpu.VMEM),
        out_shape=jax.ShapeDtypeStruct((rows, lanes), jnp.float32),
        scratch_shapes=[
            pltpu.VMEM(partial_value.shape, jnp.float32),
            pltpu.VMEM((2, pieces, rows // CUTS, lanes), jnp.float32),
            pltpu.VMEM((half, depth_size, rows, lanes), jnp.float32),
            pltpu.VMEM((max(half - 1, 1), rows, lanes), jnp.float32),
            pltpu.VMEM((rows, lanes), jnp.float32),
            pltpu.SemaphoreType.DMA,
            pltpu.SemaphoreType.DMA((2, pieces)),
            pltpu.SemaphoreType.DMA((2, pieces)),
            pltpu.SemaphoreType.DMA((pieces,)),
            pltpu.SemaphoreType.DMA((half, depth_size, CUTS)),
            pltpu.SemaphoreType.DMA((max(half - 1, 1),)),
            pltpu.SemaphoreType.DMA,
        ],
        compiler_params=pltpu.CompilerParams(collective_id=0, has_side_effects=True),
        name="exchange",
    )(slab_rank, partial_value)


def shards(block_tile, block_count, slab_rank, corner, offset, radius, emission, extinction):
    depth_size = lax.axis_size("depth")
    screen_size = lax.axis_size("screen")
    tiles_all = TILE_DEV * depth_size * screen_size
    partial_value = deposit(
        block_count, block_tile, corner, offset, radius, emission, extinction, tiles_all)
    gathered = partial_value.reshape(depth_size, screen_size, TILE_DEV * TS, 4 * TS)
    return exchange(gathered, slab_rank).reshape(TILE_DEV, TS, 4 * TS)


def solution(mesh):
    placed = (
        P("depth", "screen"),
        P("depth", "screen"),
        P(),
        P(None, "depth", "screen", None),
        P(None, "depth", "screen", None),
        P("depth", "screen", None),
        P(None, "depth", "screen", None),
        P("depth", "screen", None),
    )
    return jax.shard_map(
        shards,
        mesh=mesh,
        in_specs=placed,
        out_specs=P(("depth", "screen"), None, None),
        check_vma=False,
    )
```

```python
import functools

import jax
import jax.numpy as jnp
from jax import lax
from jax.experimental import pallas as pl
from jax.experimental.pallas import tpu as pltpu
from jax.sharding import PartitionSpec as P

TS = 32
FOOT = 16
TILE_DEV = 4
CHUNK = 256
UNROLL = 256
SPREAD = 0.125
CYCLE = 4
FLIPPED = 3
CUTS = 2
LAG = 4
VMEM_BYTES = 67043328
SPARE_BYTES = 1 << 16


def deposit_kernel(chunk, unroll, count_ref, tile_ref, corner_ref, offset_ref, radius_ref,
                   emission_ref, extinction_ref, sums_ref, square_ref, shift_ref, field_ref):
    step = pl.program_id(0)
    lanes = radius_ref.shape[-1]

    @pl.when(step == 0)
    def _():
        sums_ref[...] = jnp.zeros_like(sums_ref)

    base = step * chunk
    live = jnp.clip(count_ref[0, 0] - base, 0, chunk)

    @pl.when(live > 0)
    def _():
        lane = lax.broadcasted_iota(jnp.int32, (1, lanes), 1).astype(jnp.float32)
        stretch = jnp.exp2(lane * (SPREAD / (4 * lanes)))
        area = stretch * stretch
        undo = 1.0 / (area * area)
        radius = radius_ref[0]
        square = radius * radius
        square_ref[0] = square
        square_ref[1] = square * area
        inverse = 1.0 / square
        inverse = inverse * inverse
        inverse = inverse * inverse * undo
        shift_ref[0] = 0.5 - (corner_ref[0, 0].astype(jnp.float32) + FOOT * offset_ref[0, 0])
        shift_ref[1] = (0.5 - (corner_ref[1, 0].astype(jnp.float32) + FOOT * offset_ref[1, 0])) * stretch
        alive = lax.broadcasted_iota(jnp.int32, (chunk, lanes), 0) < live
        inverse = jnp.where(alive, inverse, 0.0)
        for channel in range(3):
            field_ref[channel] = emission_ref[channel, 0] * inverse
        field_ref[3] = extinction_ref[0] * inverse

        pixel = lax.broadcasted_iota(jnp.int32, (FOOT, lanes), 0)
        near_x = pixel.astype(jnp.float32)
        far_x = near_x + FOOT
        pixel_near = (near_x, near_x * stretch)
        pixel_far = (far_x, far_x * stretch)
        nothing = jnp.zeros((FOOT, lanes), jnp.bfloat16)
        blank = jnp.zeros((2 * FOOT, lanes), jnp.bfloat16)

        def weights(axis, row):
            near = corner_ref[axis, 0, pl.ds(row, 1), :] <= pixel
            away = jnp.where(near, pixel_near[axis], pixel_far[axis]) + shift_ref[axis, pl.ds(row, 1), :]
            bump = jnp.maximum(square_ref[axis, pl.ds(row, 1), :] - away * away, 0.0)
            return near, bump * bump

        def place(near, value):
            value = value.astype(jnp.bfloat16)
            return [jnp.where(near, value, nothing), value]

        def block(row):
            near, across = weights(0, row)
            spread = []
            for channel in range(4):
                spread += place(near, across * field_ref[channel, pl.ds(row, 1), :])
            near, down = weights(1, row)
            return jnp.concatenate(place(near, down), 0), jnp.concatenate(spread, 0)

        def group(index, carry):
            first = pl.multiple_of(index * unroll, unroll)
            products = []
            for k in range(0, unroll, 4):
                parts = [block(first + k + j) for j in range(4)]
                down = [p[0] for p in parts]
                if k // 4 % CYCLE < FLIPPED:
                    side = [p[1].T for p in parts]
                    left = jnp.concatenate([
                        jnp.concatenate([down[0], blank], 1), jnp.concatenate([down[1], blank], 1),
                        jnp.concatenate([blank, down[2]], 1), jnp.concatenate([blank, down[3]], 1)], 0)
                    across_axis, keep = 0, (0, 1, 0, 1)
                else:
                    side = [p[1] for p in parts]
                    left = jnp.concatenate([
                        jnp.concatenate([down[0], blank], 1), jnp.concatenate([blank, down[1]], 1),
                        jnp.concatenate([down[2], blank], 1), jnp.concatenate([blank, down[3]], 1)], 0)
                    across_axis, keep = 1, (0, 0, 1, 1)
                right = jnp.concatenate([jnp.concatenate(side[:2], 1), jnp.concatenate(side[2:], 1)], 0)
                product = lax.dot_general(
                    left, right, (((1,), (across_axis,)), ((), ())), preferred_element_type=jnp.float32)
                products += [product[j * TS:(j + 1) * TS, keep[j] * lanes:(keep[j] + 1) * lanes]
                             for j in range(4)]
            for k in range(unroll):
                tile = tile_ref[0, base + first + k]
                sums_ref[tile] += products[k]
            return carry

        lax.fori_loop(0, (live + unroll - 1) // unroll, group, 0)


def vmem_left(held):
    return VMEM_BYTES - 4 * held - SPARE_BYTES


def deposit(block_count, block_tile, corner, offset, radius, emission, extinction, tiles_all):
    slots, lanes = radius.shape[1:]
    chunk = min(CHUNK, slots)
    unroll = min(UNROLL, chunk)

    def at(step, count_ref):
        return jnp.minimum(step, (count_ref[0, 0] - 1) // chunk)

    def wide(step, count_ref, tile_ref):
        return (0, 0, at(step, count_ref), 0)

    def narrow(step, count_ref, tile_ref):
        return (0, at(step, count_ref), 0)

    return pl.pallas_call(
        functools.partial(deposit_kernel, chunk, unroll),
        grid_spec=pltpu.PrefetchScalarGridSpec(
            num_scalar_prefetch=2,
            grid=(slots // chunk,),
            in_specs=[
                pl.BlockSpec((2, 1, chunk, lanes), wide),
                pl.BlockSpec((2, 1, chunk, lanes), wide),
                pl.BlockSpec((1, chunk, lanes), narrow),
                pl.BlockSpec((3, 1, chunk, lanes), wide),
                pl.BlockSpec((1, chunk, lanes), narrow),
            ],
            out_specs=pl.BlockSpec(memory_space=pltpu.VMEM),
            scratch_shapes=[
                pltpu.VMEM((2, chunk, lanes), jnp.float32),
                pltpu.VMEM((2, chunk, lanes), jnp.float32),
                pltpu.VMEM((4, chunk, lanes), jnp.float32),
            ],
        ),
        out_shape=pltpu.VMEM((tiles_all, TS, 4 * TS), jnp.float32),
        compiler_params=pltpu.CompilerParams(
            vmem_limit_bytes=vmem_left(tiles_all * TS * 4 * TS), dimension_semantics=("arbitrary",)),
        name="deposit",
    )(block_count, block_tile, corner, offset, radius, emission, extinction)


def signal(barrier, device):
    pl.semaphore_signal(barrier, inc=1, device_id=device, device_id_type=pl.DeviceIdType.MESH)


def exchange_kernel(rank_ref, partial_ref, image_ref, held_ref, stack_ref, ready_ref, landed_ref,
                    send_sem, recv_sem, out_sem, in_sem, image_send_sem, image_recv_sem):
    depth_size, screen_size, rows, lanes = partial_ref.shape
    half = screen_size // 2
    part = rows // CUTS
    pieces = half * depth_size * CUTS
    edge = (screen_size - 1, 0)
    me = lax.axis_index("screen")
    slab = lax.axis_index("depth")

    at_edge = jnp.logical_or(me == 0, me == screen_size - 1)
    far = jnp.logical_and(jnp.logical_not(at_edge), jnp.where(me < half, me > 1, me < screen_size - 2))
    barrier = pltpu.get_barrier_semaphore()
    counts = []

    def greet(present, device):
        counts.append(jnp.where(present, 1, 0))

        @pl.when(present)
        def _():
            signal(barrier, device)

    greet(me > 0, {"screen": me - 1})
    greet(me < screen_size - 1, {"screen": me + 1})
    for hop in range(1, depth_size):
        greet(at_edge, {"depth": lax.rem(slab + hop, depth_size)})
    greet(far, {"screen": jnp.where(me < half, 0, screen_size - 1)})
    for other in range(2, half):
        greet(me == 0, {"screen": other})
        greet(me == screen_size - 1, {"screen": screen_size - 1 - other})
    total = counts[0]
    for count in counts[1:]:
        total = total + count
    pl.semaphore_wait(barrier, total)

    def place(side, j):
        group = j // (depth_size * CUTS)
        inside = lax.rem(j, depth_size * CUTS)
        target = lax.rem(slab + 1 + inside // CUTS, depth_size)
        owner = jnp.where(side == 1, half - 1 - group, half + group)
        return group, target, owner, lax.rem(inside, CUTS)

    def rows_of(cut):
        return pl.ds(pl.multiple_of(cut * part, part), part)

    def hop(side, j, source):
        return pltpu.make_async_remote_copy(
            src_ref=source, dst_ref=held_ref.at[side, j],
            send_sem=send_sem.at[side, j], recv_sem=recv_sem.at[side, j],
            device_id={"screen": me + 1 - 2 * side}, device_id_type=pl.DeviceIdType.MESH)

    def across_of(side, j, group, target, cut):
        return pltpu.make_async_remote_copy(
            src_ref=held_ref.at[side, j], dst_ref=stack_ref.at[group, slab, rows_of(cut)],
            send_sem=out_sem.at[j], recv_sem=in_sem.at[group, slab, cut],
            device_id={"depth": target}, device_id_type=pl.DeviceIdType.MESH)

    def arrival(group, source, cut):
        return pltpu.make_async_remote_copy(
            src_ref=held_ref.at[0, 0], dst_ref=stack_ref.at[group, source, rows_of(cut)],
            send_sem=out_sem.at[0], recv_sem=in_sem.at[group, source, cut],
            device_id={"depth": source}, device_id_type=pl.DeviceIdType.MESH)

    def handed(group, owner):
        return pltpu.make_async_remote_copy(
            src_ref=ready_ref.at[group], dst_ref=landed_ref,
            send_sem=image_send_sem.at[group], recv_sem=image_recv_sem,
            device_id={"screen": owner}, device_id_type=pl.DeviceIdType.MESH)

    for side in range(2):
        @pl.when(me == side * (screen_size - 1))
        def _(side=side):
            def launch(j, carry):
                group, target, owner, cut = place(side, j)
                hop(side, j, partial_ref.at[target, owner, rows_of(cut)]).start()
                return carry

            lax.fori_loop(0, pieces, launch, 0)

    @pl.when(jnp.logical_not(at_edge))
    def _():
        lead = jnp.where(me < half, 0, 1)
        behind = LAG * jnp.abs(2 * me - (screen_size - 1))

        def forward(side, j):
            @pl.when(jnp.logical_and(j >= 0, j < pieces))
            def _():
                group, target, owner, cut = place(side, j)
                move = hop(side, j, held_ref.at[side, j])
                move.wait_recv()
                held_ref[side, j] += partial_ref[target, owner, rows_of(cut)]
                move.start()

        def relay(i, carry):
            forward(lead, i)
            forward(1 - lead, i - behind)
            return carry

        lax.fori_loop(0, pieces + LAG * (screen_size - 1), relay, 0)

    quarter = lanes // 4
    at_once = TS

    def composite(group, out_ref):
        before = [[jnp.where(rank_ref[k] < rank_ref[j], 1.0, 0.0) for k in range(depth_size)]
                  for j in range(depth_size)]
        lane = lax.broadcasted_iota(jnp.int32, (at_once, lanes), 1)
        optical_lane = lane >= 3 * quarter

        low_lane = lax.rem(lane, 2 * FOOT) < FOOT

        def whole_rows(k, index):
            near = stack_ref[group, k, pl.ds(pl.multiple_of(index * TS, TS), FOOT)]
            total = stack_ref[group, k, pl.ds(pl.multiple_of(index * TS + FOOT, FOOT), FOOT)]
            both = jnp.concatenate([near, total - near], 0)
            return both - jnp.where(low_lane, 0.0, pltpu.roll(both, FOOT, 1))

        def step(index, carry):
            now = pl.ds(pl.multiple_of(index * at_once, at_once), at_once)
            slabs = [whole_rows(k, index) for k in range(depth_size)]
            depths = []
            for k in range(depth_size):
                optical = jnp.where(optical_lane, slabs[k], 0.0)
                optical = optical + pltpu.roll(optical, 2 * quarter, 1)
                depths.append(optical + pltpu.roll(optical, quarter, 1))
            lighting = jnp.zeros((at_once, lanes), jnp.float32)
            for j in range(depth_size):
                reach = 0.5 * depths[j]
                for k in range(depth_size):
                    if k != j:
                        reach = reach + before[j][k] * depths[k]
                lighting = lighting + jnp.exp(-reach) * slabs[j]
            whole = depths[0]
            for k in range(1, depth_size):
                whole = whole + depths[k]
            out_ref[now] = jnp.where(optical_lane, 1.0 - jnp.exp(-whole), lighting)
            return carry

        lax.fori_loop(0, rows // at_once, step, 0)

    def gather(group):
        def one(i, carry):
            source = lax.rem(slab + 1 + i // CUTS, depth_size)
            arrival(group, source, lax.rem(i, CUTS)).wait_recv()
            return carry

        lax.fori_loop(0, (depth_size - 1) * CUTS, one, 0)

    for side in range(2):
        @pl.when(me == edge[side])
        def _(side=side):
            def collect(j, carry):
                group, target, owner, cut = place(side, j)
                hop(side, j, held_ref.at[side, j]).wait_recv()

                @pl.when(target != slab)
                def _():
                    held_ref[side, j] += partial_ref[target, owner, rows_of(cut)]
                    across_of(side, j, group, target, cut).start()

                @pl.when(target == slab)
                def _():
                    stack_ref[group, slab, rows_of(cut)] = (
                        held_ref[side, j] + partial_ref[target, owner, rows_of(cut)])
                return carry

            share = depth_size * CUTS
            for group in range(half):
                lax.fori_loop(group * share, (group + 1) * share, collect, 0)
                if group > 0:
                    gather(group - 1)
                    composite(group - 1, ready_ref.at[group - 1])
                    handed(group - 1, half - group if side else half + group - 1).start()
            gather(half - 1)
            composite(half - 1, image_ref)

            def sent(j, carry):
                group, target, owner, cut = place(side, j)

                @pl.when(target != slab)
                def _():
                    across_of(side, j, group, target, cut).wait_send()
                return carry

            lax.fori_loop(0, pieces, sent, 0)
            for group in range(half - 1):
                handed(group, half - 1 - group if side else half + group).wait_send()

    @pl.when(jnp.logical_not(at_edge))
    def _():
        handed(0, me).wait_recv()
        image_ref[...] = landed_ref[...]

    for side in range(2):
        @pl.when(me != edge[side])
        def _(side=side):
            def gone(j, carry):
                hop(side, j, held_ref.at[side, j]).wait_send()
                return carry

            lax.fori_loop(0, pieces, gone, 0)


def exchange(partial_value, slab_rank):
    depth_size, screen_size, rows, lanes = partial_value.shape
    half = screen_size // 2
    pieces = half * depth_size * CUTS
    return pl.pallas_call(
        exchange_kernel,
        in_specs=[pl.BlockSpec(memory_space=pltpu.SMEM), pl.BlockSpec(memory_space=pltpu.VMEM)],
        out_specs=pl.BlockSpec(memory_space=pltpu.VMEM),
        out_shape=jax.ShapeDtypeStruct((rows, lanes), jnp.float32),
        scratch_shapes=[
            pltpu.VMEM((2, pieces, rows // CUTS, lanes), jnp.float32),
            pltpu.VMEM((half, depth_size, rows, lanes), jnp.float32),
            pltpu.VMEM((max(half - 1, 1), rows, lanes), jnp.float32),
            pltpu.VMEM((rows, lanes), jnp.float32),
            pltpu.SemaphoreType.DMA((2, pieces)),
            pltpu.SemaphoreType.DMA((2, pieces)),
            pltpu.SemaphoreType.DMA((pieces,)),
            pltpu.SemaphoreType.DMA((half, depth_size, CUTS)),
            pltpu.SemaphoreType.DMA((max(half - 1, 1),)),
            pltpu.SemaphoreType.DMA,
        ],
        compiler_params=pltpu.CompilerParams(
            vmem_limit_bytes=vmem_left(partial_value.size),
            collective_id=0, has_side_effects=True),
        name="exchange",
    )(slab_rank, pltpu.with_memory_space_constraint(partial_value, pltpu.VMEM))


def shards(block_tile, block_count, slab_rank, corner, offset, radius, emission, extinction):
    depth_size = lax.axis_size("depth")
    screen_size = lax.axis_size("screen")
    tiles_all = TILE_DEV * depth_size * screen_size
    partial_value = deposit(
        block_count, block_tile, corner, offset, radius, emission, extinction, tiles_all)
    gathered = partial_value.reshape(depth_size, screen_size, TILE_DEV * TS, 4 * TS)
    return exchange(gathered, slab_rank).reshape(TILE_DEV, TS, 4 * TS)


def solution(mesh):
    placed = (
        P("depth", "screen"),
        P("depth", "screen"),
        P(),
        P(None, "depth", "screen", None),
        P(None, "depth", "screen", None),
        P("depth", "screen", None),
        P(None, "depth", "screen", None),
        P("depth", "screen", None),
    )
    return jax.shard_map(
        shards,
        mesh=mesh,
        in_specs=placed,
        out_specs=P(("depth", "screen"), None, None),
        check_vma=False,
    )
```

```python
import functools

import jax
import jax.numpy as jnp
from jax import lax
from jax.experimental import pallas as pl
from jax.experimental.pallas import tpu as pltpu
from jax.sharding import PartitionSpec as P

TS = 32
FOOT = 16
TILE_DEV = 4
CHUNK = 256
UNROLL = 256
SPREAD = 0.125
CYCLE = 4
FLIPPED = 3
CUTS = 2
LAG = 6
VMEM_BYTES = 67043328
SPARE_BYTES = 1 << 16


def deposit_kernel(chunk, unroll, count_ref, tile_ref, corner_ref, offset_ref, radius_ref,
                   emission_ref, extinction_ref, sums_ref, square_ref, shift_ref, field_ref):
    step = pl.program_id(0)
    lanes = radius_ref.shape[-1]

    @pl.when(step == 0)
    def _():
        sums_ref[...] = jnp.zeros_like(sums_ref)

    base = step * chunk
    live = jnp.clip(count_ref[0, 0] - base, 0, chunk)

    @pl.when(live > 0)
    def _():
        lane = lax.broadcasted_iota(jnp.int32, (1, lanes), 1).astype(jnp.float32)
        stretch = jnp.exp2(lane * (SPREAD / (4 * lanes)))
        area = stretch * stretch
        undo = 1.0 / (area * area)
        radius = radius_ref[0]
        square = radius * radius
        square_ref[0] = square
        square_ref[1] = square * area
        inverse = 1.0 / square
        inverse = inverse * inverse
        inverse = inverse * inverse * undo
        shift_ref[0] = 0.5 - (corner_ref[0, 0].astype(jnp.float32) + FOOT * offset_ref[0, 0])
        shift_ref[1] = (0.5 - (corner_ref[1, 0].astype(jnp.float32) + FOOT * offset_ref[1, 0])) * stretch
        alive = lax.broadcasted_iota(jnp.int32, (chunk, lanes), 0) < live
        inverse = jnp.where(alive, inverse, 0.0)
        for channel in range(3):
            field_ref[channel] = emission_ref[channel, 0] * inverse
        field_ref[3] = extinction_ref[0] * inverse

        pixel = lax.broadcasted_iota(jnp.int32, (FOOT, lanes), 0)
        near_x = pixel.astype(jnp.float32)
        far_x = near_x + FOOT
        pixel_near = (near_x, near_x * stretch)
        pixel_far = (far_x, far_x * stretch)
        nothing = jnp.zeros((FOOT, lanes), jnp.bfloat16)
        blank = jnp.zeros((2 * FOOT, lanes), jnp.bfloat16)

        def weights(axis, row):
            near = corner_ref[axis, 0, pl.ds(row, 1), :] <= pixel
            away = jnp.where(near, pixel_near[axis], pixel_far[axis]) + shift_ref[axis, pl.ds(row, 1), :]
            bump = jnp.maximum(square_ref[axis, pl.ds(row, 1), :] - away * away, 0.0)
            return near, bump * bump

        def place(near, value):
            value = value.astype(jnp.bfloat16)
            return [jnp.where(near, value, nothing), value]

        def block(row):
            near, across = weights(0, row)
            spread = []
            for channel in range(4):
                spread += place(near, across * field_ref[channel, pl.ds(row, 1), :])
            near, down = weights(1, row)
            return jnp.concatenate(place(near, down), 0), jnp.concatenate(spread, 0)

        def group(index, carry):
            first = pl.multiple_of(index * unroll, unroll)
            products = []
            for k in range(0, unroll, 4):
                parts = [block(first + k + j) for j in range(4)]
                down = [p[0] for p in parts]
                if k // 4 % CYCLE < FLIPPED:
                    side = [p[1].T for p in parts]
                    left = jnp.concatenate([
                        jnp.concatenate([down[0], blank], 1), jnp.concatenate([down[1], blank], 1),
                        jnp.concatenate([blank, down[2]], 1), jnp.concatenate([blank, down[3]], 1)], 0)
                    across_axis, keep = 0, (0, 1, 0, 1)
                else:
                    side = [p[1] for p in parts]
                    left = jnp.concatenate([
                        jnp.concatenate([down[0], blank], 1), jnp.concatenate([blank, down[1]], 1),
                        jnp.concatenate([down[2], blank], 1), jnp.concatenate([blank, down[3]], 1)], 0)
                    across_axis, keep = 1, (0, 0, 1, 1)
                right = jnp.concatenate([jnp.concatenate(side[:2], 1), jnp.concatenate(side[2:], 1)], 0)
                product = lax.dot_general(
                    left, right, (((1,), (across_axis,)), ((), ())), preferred_element_type=jnp.float32)
                products += [product[j * TS:(j + 1) * TS, keep[j] * lanes:(keep[j] + 1) * lanes]
                             for j in range(4)]
            for k in range(unroll):
                tile = tile_ref[0, base + first + k]
                sums_ref[tile] += products[k]
            return carry

        lax.fori_loop(0, (live + unroll - 1) // unroll, group, 0)


def vmem_left(held):
    return VMEM_BYTES - 4 * held - SPARE_BYTES


def deposit(block_count, block_tile, corner, offset, radius, emission, extinction, tiles_all):
    slots, lanes = radius.shape[1:]
    chunk = min(CHUNK, slots)
    unroll = min(UNROLL, chunk)

    def at(step, count_ref):
        return jnp.minimum(step, (count_ref[0, 0] - 1) // chunk)

    def wide(step, count_ref, tile_ref):
        return (0, 0, at(step, count_ref), 0)

    def narrow(step, count_ref, tile_ref):
        return (0, at(step, count_ref), 0)

    return pl.pallas_call(
        functools.partial(deposit_kernel, chunk, unroll),
        grid_spec=pltpu.PrefetchScalarGridSpec(
            num_scalar_prefetch=2,
            grid=(slots // chunk,),
            in_specs=[
                pl.BlockSpec((2, 1, chunk, lanes), wide),
                pl.BlockSpec((2, 1, chunk, lanes), wide),
                pl.BlockSpec((1, chunk, lanes), narrow),
                pl.BlockSpec((3, 1, chunk, lanes), wide),
                pl.BlockSpec((1, chunk, lanes), narrow),
            ],
            out_specs=pl.BlockSpec(memory_space=pltpu.VMEM),
            scratch_shapes=[
                pltpu.VMEM((2, chunk, lanes), jnp.float32),
                pltpu.VMEM((2, chunk, lanes), jnp.float32),
                pltpu.VMEM((4, chunk, lanes), jnp.float32),
            ],
        ),
        out_shape=pltpu.VMEM((tiles_all, TS, 4 * TS), jnp.float32),
        compiler_params=pltpu.CompilerParams(
            vmem_limit_bytes=vmem_left(tiles_all * TS * 4 * TS), dimension_semantics=("arbitrary",)),
        name="deposit",
    )(block_count, block_tile, corner, offset, radius, emission, extinction)


def signal(barrier, device):
    pl.semaphore_signal(barrier, inc=1, device_id=device, device_id_type=pl.DeviceIdType.MESH)


def exchange_kernel(rank_ref, partial_ref, image_ref, held_ref, stack_ref, ready_ref, landed_ref,
                    send_sem, recv_sem, out_sem, in_sem, image_send_sem, image_recv_sem):
    depth_size, screen_size, rows, lanes = partial_ref.shape
    half = screen_size // 2
    part = rows // CUTS
    pieces = half * depth_size * CUTS
    edge = (screen_size - 1, 0)
    me = lax.axis_index("screen")
    slab = lax.axis_index("depth")

    at_edge = jnp.logical_or(me == 0, me == screen_size - 1)
    far = jnp.logical_and(jnp.logical_not(at_edge), jnp.where(me < half, me > 1, me < screen_size - 2))
    barrier = pltpu.get_barrier_semaphore()
    counts = []

    def greet(present, device):
        counts.append(jnp.where(present, 1, 0))

        @pl.when(present)
        def _():
            signal(barrier, device)

    greet(me > 0, {"screen": me - 1})
    greet(me < screen_size - 1, {"screen": me + 1})
    for hop in range(1, depth_size):
        greet(at_edge, {"depth": lax.rem(slab + hop, depth_size)})
    greet(far, {"screen": jnp.where(me < half, 0, screen_size - 1)})
    for other in range(2, half):
        greet(me == 0, {"screen": other})
        greet(me == screen_size - 1, {"screen": screen_size - 1 - other})
    total = counts[0]
    for count in counts[1:]:
        total = total + count
    pl.semaphore_wait(barrier, total)

    def place(side, j):
        stage = j // depth_size
        group = stage // CUTS
        target = lax.rem(slab + 1 + lax.rem(j, depth_size), depth_size)
        owner = jnp.where(side == 1, half - 1 - group, half + group)
        return group, target, owner, lax.rem(stage, CUTS)

    def rows_of(cut):
        return pl.ds(pl.multiple_of(cut * part, part), part)

    def hop(side, j, source):
        return pltpu.make_async_remote_copy(
            src_ref=source, dst_ref=held_ref.at[side, j],
            send_sem=send_sem.at[side], recv_sem=recv_sem.at[side, j],
            device_id={"screen": me + 1 - 2 * side}, device_id_type=pl.DeviceIdType.MESH)

    def across(side, j, group, target, cut):
        return pltpu.make_async_remote_copy(
            src_ref=held_ref.at[side, j], dst_ref=stack_ref.at[group, slab, rows_of(cut)],
            send_sem=out_sem, recv_sem=in_sem.at[group, cut],
            device_id={"depth": target}, device_id_type=pl.DeviceIdType.MESH)

    def handed(group, owner):
        return pltpu.make_async_remote_copy(
            src_ref=ready_ref.at[group], dst_ref=landed_ref,
            send_sem=image_send_sem.at[group], recv_sem=image_recv_sem,
            device_id={"screen": owner}, device_id_type=pl.DeviceIdType.MESH)

    for side in range(2):
        @pl.when(me == side * (screen_size - 1))
        def _(side=side):
            def launch(j, carry):
                group, target, owner, cut = place(side, j)
                hop(side, j, partial_ref.at[target, owner, rows_of(cut)]).start()
                return carry

            lax.fori_loop(0, pieces, launch, 0)

    @pl.when(jnp.logical_not(at_edge))
    def _():
        lead = jnp.where(me < half, 0, 1)
        behind = LAG * jnp.abs(2 * me - (screen_size - 1))

        def forward(side, j):
            @pl.when(jnp.logical_and(j >= 0, j < pieces))
            def _():
                group, target, owner, cut = place(side, j)
                move = hop(side, j, held_ref.at[side, j])
                move.wait_recv()
                held_ref[side, j] += partial_ref[target, owner, rows_of(cut)]
                move.start()

        def relay(i, carry):
            forward(lead, i)
            forward(1 - lead, i - behind)
            return carry

        lax.fori_loop(0, pieces + LAG * (screen_size - 1), relay, 0)

    quarter = lanes // 4

    def composite(group, cut, out_ref):
        before = [[jnp.where(rank_ref[k] < rank_ref[j], 1.0, 0.0) for k in range(depth_size)]
                  for j in range(depth_size)]
        lane = lax.broadcasted_iota(jnp.int32, (TS, lanes), 1)
        optical_lane = lane >= 3 * quarter

        low_lane = lax.rem(lane, 2 * FOOT) < FOOT

        def whole_rows(k, index):
            near = stack_ref[group, k, pl.ds(pl.multiple_of(index * TS, TS), FOOT)]
            total = stack_ref[group, k, pl.ds(pl.multiple_of(index * TS + FOOT, FOOT), FOOT)]
            both = jnp.concatenate([near, total - near], 0)
            return both - jnp.where(low_lane, 0.0, pltpu.roll(both, FOOT, 1))

        def step(index, carry):
            now = pl.ds(pl.multiple_of(index * TS, TS), TS)
            slabs = [whole_rows(k, index) for k in range(depth_size)]
            depths = []
            for k in range(depth_size):
                optical = jnp.where(optical_lane, slabs[k], 0.0)
                optical = optical + pltpu.roll(optical, 2 * quarter, 1)
                depths.append(optical + pltpu.roll(optical, quarter, 1))
            lighting = jnp.zeros((TS, lanes), jnp.float32)
            for j in range(depth_size):
                reach = 0.5 * depths[j]
                for k in range(depth_size):
                    if k != j:
                        reach = reach + before[j][k] * depths[k]
                lighting = lighting + jnp.exp(-reach) * slabs[j]
            whole = depths[0]
            for k in range(1, depth_size):
                whole = whole + depths[k]
            out_ref[now] = jnp.where(optical_lane, 1.0 - jnp.exp(-whole), lighting)
            return carry

        lax.fori_loop(cut * (part // TS), (cut + 1) * (part // TS), step, 0)

    def gather(group, cut):
        arrived = stack_ref.at[group, pl.ds(0, depth_size - 1), rows_of(cut)]
        pltpu.make_async_remote_copy(
            src_ref=arrived, dst_ref=arrived, send_sem=out_sem, recv_sem=in_sem.at[group, cut],
            device_id={"depth": lax.rem(slab + 1, depth_size)},
            device_id_type=pl.DeviceIdType.MESH).wait_recv()

    for side in range(2):
        @pl.when(me == edge[side])
        def _(side=side):
            def collect(j, carry):
                group, target, owner, cut = place(side, j)
                hop(side, j, held_ref.at[side, j]).wait_recv()

                @pl.when(target != slab)
                def _():
                    held_ref[side, j] += partial_ref[target, owner, rows_of(cut)]
                    across(side, j, group, target, cut).start()

                @pl.when(target == slab)
                def _():
                    stack_ref[group, slab, rows_of(cut)] = (
                        held_ref[side, j] + partial_ref[target, owner, rows_of(cut)])
                return carry

            def finish(stage):
                group, cut = divmod(stage, CUTS)
                gather(group, cut)
                composite(group, cut, image_ref if group == half - 1 else ready_ref.at[group])
                if group < half - 1 and cut == CUTS - 1:
                    handed(group, half - 1 - group if side else half + group).start()

            for stage in range(half * CUTS):
                lax.fori_loop(stage * depth_size, (stage + 1) * depth_size, collect, 0)
                if stage > 0:
                    finish(stage - 1)
            finish(half * CUTS - 1)

            all_sent = held_ref.at[side, pl.ds(0, half * (depth_size - 1) * CUTS)]
            pltpu.make_async_remote_copy(
                src_ref=all_sent, dst_ref=all_sent, send_sem=out_sem, recv_sem=in_sem.at[0, 0],
                device_id={"depth": lax.rem(slab + 1, depth_size)},
                device_id_type=pl.DeviceIdType.MESH).wait_send()
            for group in range(half - 1):
                handed(group, half - 1 - group if side else half + group).wait_send()

    @pl.when(jnp.logical_not(at_edge))
    def _():
        handed(0, me).wait_recv()
        image_ref[...] = landed_ref[...]

    for side in range(2):
        @pl.when(me != edge[side])
        def _(side=side):
            pltpu.make_async_remote_copy(
                src_ref=held_ref.at[side], dst_ref=held_ref.at[side],
                send_sem=send_sem.at[side], recv_sem=recv_sem.at[side, 0],
                device_id={"screen": me + 1 - 2 * side},
                device_id_type=pl.DeviceIdType.MESH).wait_send()


def exchange(partial_value, slab_rank):
    depth_size, screen_size, rows, lanes = partial_value.shape
    half = screen_size // 2
    pieces = half * depth_size * CUTS
    return pl.pallas_call(
        exchange_kernel,
        in_specs=[pl.BlockSpec(memory_space=pltpu.SMEM), pl.BlockSpec(memory_space=pltpu.VMEM)],
        out_specs=pl.BlockSpec(memory_space=pltpu.VMEM),
        out_shape=jax.ShapeDtypeStruct((rows, lanes), jnp.float32),
        scratch_shapes=[
            pltpu.VMEM((2, pieces, rows // CUTS, lanes), jnp.float32),
            pltpu.VMEM((half, depth_size, rows, lanes), jnp.float32),
            pltpu.VMEM((max(half - 1, 1), rows, lanes), jnp.float32),
            pltpu.VMEM((rows, lanes), jnp.float32),
            pltpu.SemaphoreType.DMA((2,)),
            pltpu.SemaphoreType.DMA((2, pieces)),
            pltpu.SemaphoreType.DMA,
            pltpu.SemaphoreType.DMA((half, CUTS)),
            pltpu.SemaphoreType.DMA((max(half - 1, 1),)),
            pltpu.SemaphoreType.DMA,
        ],
        compiler_params=pltpu.CompilerParams(
            vmem_limit_bytes=vmem_left(partial_value.size),
            collective_id=0, has_side_effects=True),
        name="exchange",
    )(slab_rank, pltpu.with_memory_space_constraint(partial_value, pltpu.VMEM))


def shards(block_tile, block_count, slab_rank, corner, offset, radius, emission, extinction):
    depth_size = lax.axis_size("depth")
    screen_size = lax.axis_size("screen")
    tiles_all = TILE_DEV * depth_size * screen_size
    partial_value = deposit(
        block_count, block_tile, corner, offset, radius, emission, extinction, tiles_all)
    gathered = partial_value.reshape(depth_size, screen_size, TILE_DEV * TS, 4 * TS)
    return exchange(gathered, slab_rank).reshape(TILE_DEV, TS, 4 * TS)


def solution(mesh):
    placed = (
        P("depth", "screen"),
        P("depth", "screen"),
        P(),
        P(None, "depth", "screen", None),
        P(None, "depth", "screen", None),
        P("depth", "screen", None),
        P(None, "depth", "screen", None),
        P("depth", "screen", None),
    )
    return jax.shard_map(
        shards,
        mesh=mesh,
        in_specs=placed,
        out_specs=P(("depth", "screen"), None, None),
        check_vma=False,
    )
```

```python
import functools

import jax
import jax.numpy as jnp
from jax import lax
from jax.experimental import pallas as pl
from jax.experimental.pallas import tpu as pltpu
from jax.sharding import PartitionSpec as P

TS = 32
FOOT = 16
TILE_DEV = 4
CHUNK = 256
UNROLL = 256
SPREAD = 0.125
CYCLE = 4
FLIPPED = 3
CUTS = 2
LAG = 6
VMEM_BYTES = 67043328
SPARE_BYTES = 1 << 16


def deposit_kernel(chunk, unroll, count_ref, tile_ref, corner_ref, offset_ref, radius_ref,
                   emission_ref, extinction_ref, sums_ref, square_ref, shift_ref, field_ref):
    step = pl.program_id(0)
    lanes = radius_ref.shape[-1]

    @pl.when(step == 0)
    def _():
        sums_ref[...] = jnp.zeros_like(sums_ref)

    base = step * chunk
    live = jnp.clip(count_ref[0, 0] - base, 0, chunk)

    @pl.when(live > 0)
    def _():
        lane = lax.broadcasted_iota(jnp.int32, (1, lanes), 1).astype(jnp.float32)
        stretch = jnp.exp2(lane * (SPREAD / (4 * lanes)))
        area = stretch * stretch
        undo = 1.0 / (area * area)
        radius = radius_ref[0]
        square = radius * radius
        square_ref[0] = square
        square_ref[1] = square * area
        inverse = 1.0 / square
        inverse = inverse * inverse
        inverse = inverse * inverse * undo
        shift_ref[0] = 0.5 - (corner_ref[0, 0].astype(jnp.float32) + FOOT * offset_ref[0, 0])
        shift_ref[1] = (0.5 - (corner_ref[1, 0].astype(jnp.float32) + FOOT * offset_ref[1, 0])) * stretch
        alive = lax.broadcasted_iota(jnp.int32, (chunk, lanes), 0) < live
        inverse = jnp.where(alive, inverse, 0.0)
        for channel in range(3):
            field_ref[channel] = emission_ref[channel, 0] * inverse
        field_ref[3] = extinction_ref[0] * inverse

        pixel = lax.broadcasted_iota(jnp.int32, (FOOT, lanes), 0)
        near_x = pixel.astype(jnp.float32)
        far_x = near_x + FOOT
        pixel_near = (near_x, near_x * stretch)
        pixel_far = (far_x, far_x * stretch)
        nothing = jnp.zeros((FOOT, lanes), jnp.bfloat16)
        blank = jnp.zeros((2 * FOOT, lanes), jnp.bfloat16)

        def weights(axis, row):
            near = corner_ref[axis, 0, pl.ds(row, 1), :] <= pixel
            away = jnp.where(near, pixel_near[axis], pixel_far[axis]) + shift_ref[axis, pl.ds(row, 1), :]
            bump = jnp.maximum(square_ref[axis, pl.ds(row, 1), :] - away * away, 0.0)
            return near, bump * bump

        def place(near, value):
            value = value.astype(jnp.bfloat16)
            return [jnp.where(near, value, nothing), value]

        def block(row):
            near, across = weights(0, row)
            spread = []
            for channel in range(4):
                spread += place(near, across * field_ref[channel, pl.ds(row, 1), :])
            near, down = weights(1, row)
            return jnp.concatenate(place(near, down), 0), jnp.concatenate(spread, 0)

        def group(index, carry):
            first = pl.multiple_of(index * unroll, unroll)
            products = []
            for k in range(0, unroll, 4):
                parts = [block(first + k + j) for j in range(4)]
                down = [p[0] for p in parts]
                if k // 4 % CYCLE < FLIPPED:
                    side = [p[1].T for p in parts]
                    left = jnp.concatenate([
                        jnp.concatenate([down[0], blank], 1), jnp.concatenate([down[1], blank], 1),
                        jnp.concatenate([blank, down[2]], 1), jnp.concatenate([blank, down[3]], 1)], 0)
                    across_axis, keep = 0, (0, 1, 0, 1)
                else:
                    side = [p[1] for p in parts]
                    left = jnp.concatenate([
                        jnp.concatenate([down[0], blank], 1), jnp.concatenate([blank, down[1]], 1),
                        jnp.concatenate([down[2], blank], 1), jnp.concatenate([blank, down[3]], 1)], 0)
                    across_axis, keep = 1, (0, 0, 1, 1)
                right = jnp.concatenate([jnp.concatenate(side[:2], 1), jnp.concatenate(side[2:], 1)], 0)
                product = lax.dot_general(
                    left, right, (((1,), (across_axis,)), ((), ())), preferred_element_type=jnp.float32)
                products += [product[j * TS:(j + 1) * TS, keep[j] * lanes:(keep[j] + 1) * lanes]
                             for j in range(4)]
            for k in range(unroll):
                tile = tile_ref[0, base + first + k]
                sums_ref[tile] += products[k]
            return carry

        lax.fori_loop(0, (live + unroll - 1) // unroll, group, 0)


def vmem_left(held):
    return VMEM_BYTES - 4 * held - SPARE_BYTES


def deposit(block_count, block_tile, corner, offset, radius, emission, extinction, tiles_all):
    slots, lanes = radius.shape[1:]
    chunk = min(CHUNK, slots)
    unroll = min(UNROLL, chunk)

    def at(step, count_ref):
        return jnp.minimum(step, (count_ref[0, 0] - 1) // chunk)

    def wide(step, count_ref, tile_ref):
        return (0, 0, at(step, count_ref), 0)

    def narrow(step, count_ref, tile_ref):
        return (0, at(step, count_ref), 0)

    return pl.pallas_call(
        functools.partial(deposit_kernel, chunk, unroll),
        grid_spec=pltpu.PrefetchScalarGridSpec(
            num_scalar_prefetch=2,
            grid=(slots // chunk,),
            in_specs=[
                pl.BlockSpec((2, 1, chunk, lanes), wide),
                pl.BlockSpec((2, 1, chunk, lanes), wide),
                pl.BlockSpec((1, chunk, lanes), narrow),
                pl.BlockSpec((3, 1, chunk, lanes), wide),
                pl.BlockSpec((1, chunk, lanes), narrow),
            ],
            out_specs=pl.BlockSpec(memory_space=pltpu.VMEM),
            scratch_shapes=[
                pltpu.VMEM((2, chunk, lanes), jnp.float32),
                pltpu.VMEM((2, chunk, lanes), jnp.float32),
                pltpu.VMEM((4, chunk, lanes), jnp.float32),
            ],
        ),
        out_shape=pltpu.VMEM((tiles_all, TS, 4 * TS), jnp.float32),
        compiler_params=pltpu.CompilerParams(
            vmem_limit_bytes=vmem_left(tiles_all * TS * 4 * TS), dimension_semantics=("arbitrary",)),
        name="deposit",
    )(block_count, block_tile, corner, offset, radius, emission, extinction)


def signal(barrier, device):
    pl.semaphore_signal(barrier, inc=1, device_id=device, device_id_type=pl.DeviceIdType.MESH)


def exchange_kernel(rank_ref, partial_ref, image_ref, held_ref, stack_ref, ready_ref, landed_ref,
                    send_sem, recv_sem, out_sem, in_sem, image_send_sem, image_recv_sem, ready_sem):
    depth_size, screen_size, rows, lanes = partial_ref.shape
    half = screen_size // 2
    part = rows // CUTS
    pieces = half * depth_size * CUTS
    edge = (screen_size - 1, 0)
    me = lax.axis_index("screen")
    slab = lax.axis_index("depth")

    at_edge = jnp.logical_or(me == 0, me == screen_size - 1)
    middle = jnp.logical_not(at_edge)
    home = jnp.where(me < half, 0, screen_size - 1)
    beside = jnp.logical_or(me == 1, me == screen_size - 2)
    barrier = pltpu.get_barrier_semaphore()

    def greet(present, device):
        @pl.when(present)
        def _():
            signal(barrier, device)

    greet(me > 1, {"screen": me - 1})
    greet(me < screen_size - 2, {"screen": me + 1})
    for hop in range(1, depth_size):
        greet(at_edge, {"depth": lax.rem(slab + hop, depth_size)})
    greet(jnp.logical_and(middle, jnp.logical_not(beside)), {"screen": home})

    @pl.when(middle)
    def _():
        pl.semaphore_wait(barrier, 2)

    @pl.when(beside)
    def _():
        signal(ready_sem, {"screen": home})

    @pl.when(at_edge)
    def _():
        pl.semaphore_wait(ready_sem, 1)

    def place(side, j):
        stage = j // depth_size
        group = stage // CUTS
        target = lax.rem(slab + 1 + lax.rem(j, depth_size), depth_size)
        owner = jnp.where(side == 1, half - 1 - group, half + group)
        return group, target, owner, lax.rem(stage, CUTS)

    def rows_of(cut):
        return pl.ds(pl.multiple_of(cut * part, part), part)

    def hop(side, j, source):
        return pltpu.make_async_remote_copy(
            src_ref=source, dst_ref=held_ref.at[side, j],
            send_sem=send_sem.at[side], recv_sem=recv_sem.at[side, j],
            device_id={"screen": me + 1 - 2 * side}, device_id_type=pl.DeviceIdType.MESH)

    def across(side, j, group, target, cut):
        return pltpu.make_async_remote_copy(
            src_ref=held_ref.at[side, j], dst_ref=stack_ref.at[group, slab, rows_of(cut)],
            send_sem=out_sem, recv_sem=in_sem.at[group, cut],
            device_id={"depth": target}, device_id_type=pl.DeviceIdType.MESH)

    def handed(group, owner):
        return pltpu.make_async_remote_copy(
            src_ref=ready_ref.at[group], dst_ref=landed_ref,
            send_sem=image_send_sem.at[group], recv_sem=image_recv_sem,
            device_id={"screen": owner}, device_id_type=pl.DeviceIdType.MESH)

    for side in range(2):
        @pl.when(me == side * (screen_size - 1))
        def _(side=side):
            def launch(j, carry):
                group, target, owner, cut = place(side, j)
                hop(side, j, partial_ref.at[target, owner, rows_of(cut)]).start()
                return carry

            lax.fori_loop(0, pieces, launch, 0)

    @pl.when(middle)
    def _():
        lead = jnp.where(me < half, 0, 1)
        behind = LAG * jnp.abs(2 * me - (screen_size - 1))

        def forward(side, j):
            @pl.when(jnp.logical_and(j >= 0, j < pieces))
            def _():
                group, target, owner, cut = place(side, j)
                move = hop(side, j, held_ref.at[side, j])
                move.wait_recv()
                held_ref[side, j] += partial_ref[target, owner, rows_of(cut)]
                move.start()

        def relay(i, carry):
            forward(lead, i)
            forward(1 - lead, i - behind)
            return carry

        lax.fori_loop(0, pieces + LAG * (screen_size - 1), relay, 0)

    quarter = lanes // 4

    def composite(group, cut, out_ref):
        before = [[jnp.where(rank_ref[k] < rank_ref[j], 1.0, 0.0) for k in range(depth_size)]
                  for j in range(depth_size)]
        lane = lax.broadcasted_iota(jnp.int32, (TS, lanes), 1)
        optical_lane = lane >= 3 * quarter

        low_lane = lax.rem(lane, 2 * FOOT) < FOOT

        def whole_rows(k, index):
            near = stack_ref[group, k, pl.ds(pl.multiple_of(index * TS, TS), FOOT)]
            total = stack_ref[group, k, pl.ds(pl.multiple_of(index * TS + FOOT, FOOT), FOOT)]
            both = jnp.concatenate([near, total - near], 0)
            return both - jnp.where(low_lane, 0.0, pltpu.roll(both, FOOT, 1))

        def step(index, carry):
            now = pl.ds(pl.multiple_of(index * TS, TS), TS)
            slabs = [whole_rows(k, index) for k in range(depth_size)]
            depths = []
            for k in range(depth_size):
                optical = jnp.where(optical_lane, slabs[k], 0.0)
                optical = optical + pltpu.roll(optical, 2 * quarter, 1)
                depths.append(optical + pltpu.roll(optical, quarter, 1))
            lighting = jnp.zeros((TS, lanes), jnp.float32)
            for j in range(depth_size):
                reach = 0.5 * depths[j]
                for k in range(depth_size):
                    if k != j:
                        reach = reach + before[j][k] * depths[k]
                lighting = lighting + jnp.exp(-reach) * slabs[j]
            whole = depths[0]
            for k in range(1, depth_size):
                whole = whole + depths[k]
            out_ref[now] = jnp.where(optical_lane, 1.0 - jnp.exp(-whole), lighting)
            return carry

        lax.fori_loop(cut * (part // TS), (cut + 1) * (part // TS), step, 0)

    def gather(group, cut):
        arrived = stack_ref.at[group, pl.ds(0, depth_size - 1), rows_of(cut)]
        pltpu.make_async_remote_copy(
            src_ref=arrived, dst_ref=arrived, send_sem=out_sem, recv_sem=in_sem.at[group, cut],
            device_id={"depth": lax.rem(slab + 1, depth_size)},
            device_id_type=pl.DeviceIdType.MESH).wait_recv()

    for side in range(2):
        @pl.when(me == edge[side])
        def _(side=side):
            def collect(j, carry):
                group, target, owner, cut = place(side, j)
                hop(side, j, held_ref.at[side, j]).wait_recv()

                @pl.when(target != slab)
                def _():
                    held_ref[side, j] += partial_ref[target, owner, rows_of(cut)]
                    across(side, j, group, target, cut).start()

                @pl.when(target == slab)
                def _():
                    stack_ref[group, slab, rows_of(cut)] = (
                        held_ref[side, j] + partial_ref[target, owner, rows_of(cut)])
                return carry

            def finish(stage):
                group, cut = divmod(stage, CUTS)
                gather(group, cut)
                composite(group, cut, image_ref if group == half - 1 else ready_ref.at[group])
                if group < half - 1 and cut == CUTS - 1:
                    handed(group, half - 1 - group if side else half + group).start()

            pl.semaphore_wait(barrier, depth_size - 1 + max(half - 2, 0))
            for stage in range(half * CUTS):
                lax.fori_loop(stage * depth_size, (stage + 1) * depth_size, collect, 0)
                if stage > 0:
                    finish(stage - 1)
            finish(half * CUTS - 1)

            all_sent = held_ref.at[side, pl.ds(0, half * (depth_size - 1) * CUTS)]
            pltpu.make_async_remote_copy(
                src_ref=all_sent, dst_ref=all_sent, send_sem=out_sem, recv_sem=in_sem.at[0, 0],
                device_id={"depth": lax.rem(slab + 1, depth_size)},
                device_id_type=pl.DeviceIdType.MESH).wait_send()
            for group in range(half - 1):
                handed(group, half - 1 - group if side else half + group).wait_send()

    @pl.when(middle)
    def _():
        handed(0, me).wait_recv()
        image_ref[...] = landed_ref[...]

    for side in range(2):
        @pl.when(me != edge[side])
        def _(side=side):
            pltpu.make_async_remote_copy(
                src_ref=held_ref.at[side], dst_ref=held_ref.at[side],
                send_sem=send_sem.at[side], recv_sem=recv_sem.at[side, 0],
                device_id={"screen": me + 1 - 2 * side},
                device_id_type=pl.DeviceIdType.MESH).wait_send()


def exchange(partial_value, slab_rank):
    depth_size, screen_size, rows, lanes = partial_value.shape
    half = screen_size // 2
    pieces = half * depth_size * CUTS
    return pl.pallas_call(
        exchange_kernel,
        in_specs=[pl.BlockSpec(memory_space=pltpu.SMEM), pl.BlockSpec(memory_space=pltpu.VMEM)],
        out_specs=pl.BlockSpec(memory_space=pltpu.VMEM),
        out_shape=jax.ShapeDtypeStruct((rows, lanes), jnp.float32),
        scratch_shapes=[
            pltpu.VMEM((2, pieces, rows // CUTS, lanes), jnp.float32),
            pltpu.VMEM((half, depth_size, rows, lanes), jnp.float32),
            pltpu.VMEM((max(half - 1, 1), rows, lanes), jnp.float32),
            pltpu.VMEM((rows, lanes), jnp.float32),
            pltpu.SemaphoreType.DMA((2,)),
            pltpu.SemaphoreType.DMA((2, pieces)),
            pltpu.SemaphoreType.DMA,
            pltpu.SemaphoreType.DMA((half, CUTS)),
            pltpu.SemaphoreType.DMA((max(half - 1, 1),)),
            pltpu.SemaphoreType.DMA,
            pltpu.SemaphoreType.REGULAR,
        ],
        compiler_params=pltpu.CompilerParams(
            vmem_limit_bytes=vmem_left(partial_value.size),
            collective_id=0, has_side_effects=True),
        name="exchange",
    )(slab_rank, pltpu.with_memory_space_constraint(partial_value, pltpu.VMEM))


def shards(block_tile, block_count, slab_rank, corner, offset, radius, emission, extinction):
    depth_size = lax.axis_size("depth")
    screen_size = lax.axis_size("screen")
    tiles_all = TILE_DEV * depth_size * screen_size
    partial_value = deposit(
        block_count, block_tile, corner, offset, radius, emission, extinction, tiles_all)
    gathered = partial_value.reshape(depth_size, screen_size, TILE_DEV * TS, 4 * TS)
    return exchange(gathered, slab_rank).reshape(TILE_DEV, TS, 4 * TS)


def solution(mesh):
    placed = (
        P("depth", "screen"),
        P("depth", "screen"),
        P(),
        P(None, "depth", "screen", None),
        P(None, "depth", "screen", None),
        P("depth", "screen", None),
        P(None, "depth", "screen", None),
        P("depth", "screen", None),
    )
    return jax.shard_map(
        shards,
        mesh=mesh,
        in_specs=placed,
        out_specs=P(("depth", "screen"), None, None),
        check_vma=False,
    )
```

```python
import functools

import jax
import jax.numpy as jnp
from jax import lax
from jax.experimental import pallas as pl
from jax.experimental.pallas import tpu as pltpu
from jax.sharding import PartitionSpec as P

TS = 32
FOOT = 16
TILE_DEV = 4
CHUNK = 512
UNROLL = 512
SPREAD = 0.125
CYCLE = 4
FLIPPED = 3
CUTS = 2
LAG = 6
VMEM_BYTES = 67043328
SPARE_BYTES = 1 << 19


def deposit_kernel(chunk, unroll, count_ref, tile_ref, corner_ref, offset_ref, radius_ref,
                   emission_ref, extinction_ref, sums_ref, square_ref, shift_ref, field_ref):
    step = pl.program_id(0)
    lanes = radius_ref.shape[-1]

    @pl.when(step == 0)
    def _():
        sums_ref[...] = jnp.zeros_like(sums_ref)

    base = step * chunk
    live = jnp.clip(count_ref[0, 0] - base, 0, chunk)

    @pl.when(live > 0)
    def _():
        lane = lax.broadcasted_iota(jnp.int32, (1, lanes), 1).astype(jnp.float32)
        stretch = jnp.exp2(lane * (SPREAD / (4 * lanes)))
        area = stretch * stretch
        undo = 1.0 / (area * area)
        radius = radius_ref[0]
        square = radius * radius
        square_ref[0] = square
        square_ref[1] = square * area
        inverse = 1.0 / square
        inverse = inverse * inverse
        inverse = inverse * inverse * undo
        shift_ref[0] = 0.5 - (corner_ref[0, 0].astype(jnp.float32) + FOOT * offset_ref[0, 0])
        shift_ref[1] = (0.5 - (corner_ref[1, 0].astype(jnp.float32) + FOOT * offset_ref[1, 0])) * stretch
        alive = lax.broadcasted_iota(jnp.int32, (chunk, lanes), 0) < live
        inverse = jnp.where(alive, inverse, 0.0)
        for channel in range(3):
            field_ref[channel] = emission_ref[channel, 0] * inverse
        field_ref[3] = extinction_ref[0] * inverse

        pixel = lax.broadcasted_iota(jnp.int32, (FOOT, lanes), 0)
        near_x = pixel.astype(jnp.float32)
        far_x = near_x + FOOT
        pixel_near = (near_x, near_x * stretch)
        pixel_far = (far_x, far_x * stretch)
        nothing = jnp.zeros((FOOT, lanes), jnp.bfloat16)
        blank = jnp.zeros((2 * FOOT, lanes), jnp.bfloat16)

        def weights(axis, row):
            near = corner_ref[axis, 0, pl.ds(row, 1), :] <= pixel
            away = jnp.where(near, pixel_near[axis], pixel_far[axis]) + shift_ref[axis, pl.ds(row, 1), :]
            bump = jnp.maximum(square_ref[axis, pl.ds(row, 1), :] - away * away, 0.0)
            return near, bump * bump

        def place(near, value):
            value = value.astype(jnp.bfloat16)
            return [jnp.where(near, value, nothing), value]

        def block(row):
            near, across = weights(0, row)
            spread = []
            for channel in range(4):
                spread += place(near, across * field_ref[channel, pl.ds(row, 1), :])
            near, down = weights(1, row)
            return jnp.concatenate(place(near, down), 0), jnp.concatenate(spread, 0)

        def group(index, carry):
            first = pl.multiple_of(index * unroll, unroll)
            products = []
            for k in range(0, unroll, 4):
                parts = [block(first + k + j) for j in range(4)]
                down = [p[0] for p in parts]
                if k // 4 % CYCLE < FLIPPED:
                    side = [p[1].T for p in parts]
                    left = jnp.concatenate([
                        jnp.concatenate([down[0], blank], 1), jnp.concatenate([down[1], blank], 1),
                        jnp.concatenate([blank, down[2]], 1), jnp.concatenate([blank, down[3]], 1)], 0)
                    across_axis, keep = 0, (0, 1, 0, 1)
                else:
                    side = [p[1] for p in parts]
                    left = jnp.concatenate([
                        jnp.concatenate([down[0], blank], 1), jnp.concatenate([blank, down[1]], 1),
                        jnp.concatenate([down[2], blank], 1), jnp.concatenate([blank, down[3]], 1)], 0)
                    across_axis, keep = 1, (0, 0, 1, 1)
                right = jnp.concatenate([jnp.concatenate(side[:2], 1), jnp.concatenate(side[2:], 1)], 0)
                product = lax.dot_general(
                    left, right, (((1,), (across_axis,)), ((), ())), preferred_element_type=jnp.float32)
                products += [product[j * TS:(j + 1) * TS, keep[j] * lanes:(keep[j] + 1) * lanes]
                             for j in range(4)]
            for k in range(unroll):
                tile = tile_ref[0, base + first + k]
                sums_ref[tile] += products[k]
            return carry

        lax.fori_loop(0, (live + unroll - 1) // unroll, group, 0)


def vmem_left(held):
    return VMEM_BYTES - 4 * held - SPARE_BYTES


def deposit(block_count, block_tile, corner, offset, radius, emission, extinction, tiles_all):
    slots, lanes = radius.shape[1:]
    chunk = min(CHUNK, slots)
    unroll = min(UNROLL, chunk)

    def at(step, count_ref):
        return jnp.minimum(step, (count_ref[0, 0] - 1) // chunk)

    def wide(step, count_ref, tile_ref):
        return (0, 0, at(step, count_ref), 0)

    def narrow(step, count_ref, tile_ref):
        return (0, at(step, count_ref), 0)

    return pl.pallas_call(
        functools.partial(deposit_kernel, chunk, unroll),
        grid_spec=pltpu.PrefetchScalarGridSpec(
            num_scalar_prefetch=2,
            grid=(slots // chunk,),
            in_specs=[
                pl.BlockSpec((2, 1, chunk, lanes), wide),
                pl.BlockSpec((2, 1, chunk, lanes), wide),
                pl.BlockSpec((1, chunk, lanes), narrow),
                pl.BlockSpec((3, 1, chunk, lanes), wide),
                pl.BlockSpec((1, chunk, lanes), narrow),
            ],
            out_specs=pl.BlockSpec(memory_space=pltpu.VMEM),
            scratch_shapes=[
                pltpu.VMEM((2, chunk, lanes), jnp.float32),
                pltpu.VMEM((2, chunk, lanes), jnp.float32),
                pltpu.VMEM((4, chunk, lanes), jnp.float32),
            ],
        ),
        out_shape=pltpu.VMEM((tiles_all, TS, 4 * TS), jnp.float32),
        compiler_params=pltpu.CompilerParams(
            vmem_limit_bytes=vmem_left(tiles_all * TS * 4 * TS), dimension_semantics=("arbitrary",)),
        name="deposit",
    )(block_count, block_tile, corner, offset, radius, emission, extinction)


def signal(barrier, device):
    pl.semaphore_signal(barrier, inc=1, device_id=device, device_id_type=pl.DeviceIdType.MESH)


def exchange_kernel(rank_ref, partial_ref, image_ref, held_ref, stack_ref, ready_ref, landed_ref,
                    send_sem, recv_sem, out_sem, in_sem, image_send_sem, image_recv_sem, ready_sem):
    depth_size, screen_size, rows, lanes = partial_ref.shape
    half = screen_size // 2
    part = rows // CUTS
    pieces = half * depth_size * CUTS
    edge = (screen_size - 1, 0)
    me = lax.axis_index("screen")
    slab = lax.axis_index("depth")

    at_edge = jnp.logical_or(me == 0, me == screen_size - 1)
    middle = jnp.logical_not(at_edge)
    home = jnp.where(me < half, 0, screen_size - 1)
    beside = jnp.logical_or(me == 1, me == screen_size - 2)
    barrier = pltpu.get_barrier_semaphore()

    def greet(present, device):
        @pl.when(present)
        def _():
            signal(barrier, device)

    greet(me > 1, {"screen": me - 1})
    greet(me < screen_size - 2, {"screen": me + 1})
    for hop in range(1, depth_size):
        greet(at_edge, {"depth": lax.rem(slab + hop, depth_size)})
    greet(jnp.logical_and(middle, jnp.logical_not(beside)), {"screen": home})

    @pl.when(middle)
    def _():
        pl.semaphore_wait(barrier, 2)

    @pl.when(beside)
    def _():
        signal(ready_sem, {"screen": home})

    @pl.when(at_edge)
    def _():
        pl.semaphore_wait(ready_sem, 1)

    def place(side, j):
        stage = j // depth_size
        group = stage // CUTS
        target = lax.rem(slab + 1 + lax.rem(j, depth_size), depth_size)
        owner = jnp.where(side == 1, half - 1 - group, half + group)
        return group, target, owner, lax.rem(stage, CUTS)

    def rows_of(cut):
        return pl.ds(pl.multiple_of(cut * part, part), part)

    def hop(side, j, source):
        return pltpu.make_async_remote_copy(
            src_ref=source, dst_ref=held_ref.at[side, j],
            send_sem=send_sem.at[side], recv_sem=recv_sem.at[side, j],
            device_id={"screen": me + 1 - 2 * side}, device_id_type=pl.DeviceIdType.MESH)

    def across(side, j, group, target, cut):
        return pltpu.make_async_remote_copy(
            src_ref=held_ref.at[side, j], dst_ref=stack_ref.at[group, slab, rows_of(cut)],
            send_sem=out_sem, recv_sem=in_sem.at[group, cut],
            device_id={"depth": target}, device_id_type=pl.DeviceIdType.MESH)

    def handed(group, owner):
        return pltpu.make_async_remote_copy(
            src_ref=ready_ref.at[group], dst_ref=landed_ref,
            send_sem=image_send_sem.at[group], recv_sem=image_recv_sem,
            device_id={"screen": owner}, device_id_type=pl.DeviceIdType.MESH)

    for side in range(2):
        @pl.when(me == side * (screen_size - 1))
        def _(side=side):
            def launch(j, carry):
                group, target, owner, cut = place(side, j)
                hop(side, j, partial_ref.at[target, owner, rows_of(cut)]).start()
                return carry

            lax.fori_loop(0, pieces, launch, 0)

    @pl.when(middle)
    def _():
        lead = jnp.where(me < half, 0, 1)
        behind = LAG * jnp.abs(2 * me - (screen_size - 1))

        def forward(side, j):
            @pl.when(jnp.logical_and(j >= 0, j < pieces))
            def _():
                group, target, owner, cut = place(side, j)
                move = hop(side, j, held_ref.at[side, j])
                move.wait_recv()
                held_ref[side, j] += partial_ref[target, owner, rows_of(cut)]
                move.start()

        def relay(i, carry):
            forward(lead, i)
            forward(1 - lead, i - behind)
            return carry

        lax.fori_loop(0, pieces + LAG * (screen_size - 1), relay, 0)

    quarter = lanes // 4

    def composite(group, cut, out_ref):
        before = [[jnp.where(rank_ref[k] < rank_ref[j], 1.0, 0.0) for k in range(depth_size)]
                  for j in range(depth_size)]
        lane = lax.broadcasted_iota(jnp.int32, (TS, lanes), 1)
        optical_lane = lane >= 3 * quarter

        low_lane = lax.rem(lane, 2 * FOOT) < FOOT

        def whole_rows(k, index):
            near = stack_ref[group, k, pl.ds(pl.multiple_of(index * TS, TS), FOOT)]
            total = stack_ref[group, k, pl.ds(pl.multiple_of(index * TS + FOOT, FOOT), FOOT)]
            both = jnp.concatenate([near, total - near], 0)
            return both - jnp.where(low_lane, 0.0, pltpu.roll(both, FOOT, 1))

        def step(index, carry):
            now = pl.ds(pl.multiple_of(index * TS, TS), TS)
            slabs = [whole_rows(k, index) for k in range(depth_size)]
            depths = []
            for k in range(depth_size):
                optical = jnp.where(optical_lane, slabs[k], 0.0)
                optical = optical + pltpu.roll(optical, 2 * quarter, 1)
                depths.append(optical + pltpu.roll(optical, quarter, 1))
            lighting = jnp.zeros((TS, lanes), jnp.float32)
            for j in range(depth_size):
                reach = 0.5 * depths[j]
                for k in range(depth_size):
                    if k != j:
                        reach = reach + before[j][k] * depths[k]
                lighting = lighting + jnp.exp(-reach) * slabs[j]
            whole = depths[0]
            for k in range(1, depth_size):
                whole = whole + depths[k]
            out_ref[now] = jnp.where(optical_lane, 1.0 - jnp.exp(-whole), lighting)
            return carry

        lax.fori_loop(cut * (part // TS), (cut + 1) * (part // TS), step, 0)

    def gather(group, cut):
        arrived = stack_ref.at[group, pl.ds(0, depth_size - 1), rows_of(cut)]
        pltpu.make_async_remote_copy(
            src_ref=arrived, dst_ref=arrived, send_sem=out_sem, recv_sem=in_sem.at[group, cut],
            device_id={"depth": lax.rem(slab + 1, depth_size)},
            device_id_type=pl.DeviceIdType.MESH).wait_recv()

    for side in range(2):
        @pl.when(me == edge[side])
        def _(side=side):
            def collect(j, carry):
                group, target, owner, cut = place(side, j)
                hop(side, j, held_ref.at[side, j]).wait_recv()

                @pl.when(target != slab)
                def _():
                    held_ref[side, j] += partial_ref[target, owner, rows_of(cut)]
                    across(side, j, group, target, cut).start()

                @pl.when(target == slab)
                def _():
                    stack_ref[group, slab, rows_of(cut)] = (
                        held_ref[side, j] + partial_ref[target, owner, rows_of(cut)])
                return carry

            def finish(stage):
                group, cut = divmod(stage, CUTS)
                gather(group, cut)
                composite(group, cut, image_ref if group == half - 1 else ready_ref.at[group])
                if group < half - 1 and cut == CUTS - 1:
                    handed(group, half - 1 - group if side else half + group).start()

            pl.semaphore_wait(barrier, depth_size - 1 + max(half - 2, 0))
            for stage in range(half * CUTS):
                lax.fori_loop(stage * depth_size, (stage + 1) * depth_size, collect, 0)
                if stage > 0:
                    finish(stage - 1)
            finish(half * CUTS - 1)

            all_sent = held_ref.at[side, pl.ds(0, half * (depth_size - 1) * CUTS)]
            pltpu.make_async_remote_copy(
                src_ref=all_sent, dst_ref=all_sent, send_sem=out_sem, recv_sem=in_sem.at[0, 0],
                device_id={"depth": lax.rem(slab + 1, depth_size)},
                device_id_type=pl.DeviceIdType.MESH).wait_send()
            for group in range(half - 1):
                handed(group, half - 1 - group if side else half + group).wait_send()

    @pl.when(middle)
    def _():
        handed(0, me).wait_recv()
        image_ref[...] = landed_ref[...]

    for side in range(2):
        @pl.when(me != edge[side])
        def _(side=side):
            pltpu.make_async_remote_copy(
                src_ref=held_ref.at[side], dst_ref=held_ref.at[side],
                send_sem=send_sem.at[side], recv_sem=recv_sem.at[side, 0],
                device_id={"screen": me + 1 - 2 * side},
                device_id_type=pl.DeviceIdType.MESH).wait_send()


def exchange(partial_value, slab_rank):
    depth_size, screen_size, rows, lanes = partial_value.shape
    half = screen_size // 2
    pieces = half * depth_size * CUTS
    return pl.pallas_call(
        exchange_kernel,
        in_specs=[pl.BlockSpec(memory_space=pltpu.SMEM), pl.BlockSpec(memory_space=pltpu.VMEM)],
        out_specs=pl.BlockSpec(memory_space=pltpu.VMEM),
        out_shape=pltpu.VMEM((rows, lanes), jnp.float32),
        scratch_shapes=[
            pltpu.VMEM((2, pieces, rows // CUTS, lanes), jnp.float32),
            pltpu.VMEM((half, depth_size, rows, lanes), jnp.float32),
            pltpu.VMEM((max(half - 1, 1), rows, lanes), jnp.float32),
            pltpu.VMEM((rows, lanes), jnp.float32),
            pltpu.SemaphoreType.DMA((2,)),
            pltpu.SemaphoreType.DMA((2, pieces)),
            pltpu.SemaphoreType.DMA,
            pltpu.SemaphoreType.DMA((half, CUTS)),
            pltpu.SemaphoreType.DMA((max(half - 1, 1),)),
            pltpu.SemaphoreType.DMA,
            pltpu.SemaphoreType.REGULAR,
        ],
        compiler_params=pltpu.CompilerParams(
            vmem_limit_bytes=vmem_left(partial_value.size),
            collective_id=0, has_side_effects=True),
        name="exchange",
    )(slab_rank, pltpu.with_memory_space_constraint(partial_value, pltpu.VMEM))


def shards(block_tile, block_count, slab_rank, corner, offset, radius, emission, extinction):
    depth_size = lax.axis_size("depth")
    screen_size = lax.axis_size("screen")
    tiles_all = TILE_DEV * depth_size * screen_size
    partial_value = deposit(
        block_count, block_tile, corner, offset, radius, emission, extinction, tiles_all)
    gathered = partial_value.reshape(depth_size, screen_size, TILE_DEV * TS, 4 * TS)
    return exchange(gathered, slab_rank).reshape(TILE_DEV, TS, 4 * TS)


def solution(mesh):
    placed = (
        P("depth", "screen"),
        P("depth", "screen"),
        P(),
        P(None, "depth", "screen", None),
        P(None, "depth", "screen", None),
        P("depth", "screen", None),
        P(None, "depth", "screen", None),
        P("depth", "screen", None),
    )
    return jax.shard_map(
        shards,
        mesh=mesh,
        in_specs=placed,
        out_specs=P(("depth", "screen"), None, None),
        check_vma=False,
    )
```

```python
import functools

import jax
import jax.numpy as jnp
from jax import lax
from jax.experimental import pallas as pl
from jax.experimental.pallas import tpu as pltpu
from jax.sharding import PartitionSpec as P

TS = 32
FOOT = 16
TILE_DEV = 4
CHUNK = 512
UNROLL = 512
SPREAD = 0.125
CYCLE = 4
FLIPPED = 3
CUTS = 2
LAG = 7
VMEM_BYTES = 67043328
SPARE_BYTES = 1 << 19


def deposit_kernel(chunk, unroll, count_ref, tile_ref, corner_ref, offset_ref, radius_ref,
                   emission_ref, extinction_ref, sums_ref, square_ref, shift_ref, field_ref):
    step = pl.program_id(0)
    lanes = radius_ref.shape[-1]

    @pl.when(step == 0)
    def _():
        sums_ref[...] = jnp.zeros_like(sums_ref)

    base = step * chunk
    live = jnp.clip(count_ref[0, 0] - base, 0, chunk)

    @pl.when(live > 0)
    def _():
        lane = lax.broadcasted_iota(jnp.int32, (1, lanes), 1).astype(jnp.float32)
        stretch = jnp.exp2(lane * (SPREAD / (4 * lanes)))
        area = stretch * stretch
        undo = 1.0 / (area * area)
        radius = radius_ref[0]
        square = radius * radius
        square_ref[0] = square
        square_ref[1] = square * area
        inverse = 1.0 / square
        inverse = inverse * inverse
        inverse = inverse * inverse * undo
        shift_ref[0] = 0.5 - (corner_ref[0, 0].astype(jnp.float32) + FOOT * offset_ref[0, 0])
        shift_ref[1] = (0.5 - (corner_ref[1, 0].astype(jnp.float32) + FOOT * offset_ref[1, 0])) * stretch
        alive = lax.broadcasted_iota(jnp.int32, (chunk, lanes), 0) < live
        inverse = jnp.where(alive, inverse, 0.0)
        for channel in range(3):
            field_ref[channel] = emission_ref[channel, 0] * inverse
        field_ref[3] = extinction_ref[0] * inverse

        pixel = lax.broadcasted_iota(jnp.int32, (FOOT, lanes), 0)
        near_x = pixel.astype(jnp.float32)
        far_x = near_x + FOOT
        pixel_near = (near_x, near_x * stretch)
        pixel_far = (far_x, far_x * stretch)
        nothing = jnp.zeros((FOOT, lanes), jnp.bfloat16)
        blank = jnp.zeros((2 * FOOT, lanes), jnp.bfloat16)

        def weights(axis, row):
            near = corner_ref[axis, 0, pl.ds(row, 1), :] <= pixel
            away = jnp.where(near, pixel_near[axis], pixel_far[axis]) + shift_ref[axis, pl.ds(row, 1), :]
            bump = jnp.maximum(square_ref[axis, pl.ds(row, 1), :] - away * away, 0.0)
            return near, bump * bump

        def place(near, value):
            value = value.astype(jnp.bfloat16)
            return [jnp.where(near, value, nothing), value]

        def block(row):
            near, across = weights(0, row)
            spread = []
            for channel in range(4):
                spread += place(near, across * field_ref[channel, pl.ds(row, 1), :])
            near, down = weights(1, row)
            return jnp.concatenate(place(near, down), 0), jnp.concatenate(spread, 0)

        def group(index, carry):
            first = pl.multiple_of(index * unroll, unroll)
            products = []
            for k in range(0, unroll, 4):
                parts = [block(first + k + j) for j in range(4)]
                down = [p[0] for p in parts]
                if k // 4 % CYCLE < FLIPPED:
                    side = [p[1].T for p in parts]
                    left = jnp.concatenate([
                        jnp.concatenate([down[0], blank], 1), jnp.concatenate([down[1], blank], 1),
                        jnp.concatenate([blank, down[2]], 1), jnp.concatenate([blank, down[3]], 1)], 0)
                    across_axis, keep = 0, (0, 1, 0, 1)
                else:
                    side = [p[1] for p in parts]
                    left = jnp.concatenate([
                        jnp.concatenate([down[0], blank], 1), jnp.concatenate([blank, down[1]], 1),
                        jnp.concatenate([down[2], blank], 1), jnp.concatenate([blank, down[3]], 1)], 0)
                    across_axis, keep = 1, (0, 0, 1, 1)
                right = jnp.concatenate([jnp.concatenate(side[:2], 1), jnp.concatenate(side[2:], 1)], 0)
                product = lax.dot_general(
                    left, right, (((1,), (across_axis,)), ((), ())), preferred_element_type=jnp.float32)
                products += [product[j * TS:(j + 1) * TS, keep[j] * lanes:(keep[j] + 1) * lanes]
                             for j in range(4)]
            for k in range(unroll):
                tile = tile_ref[0, base + first + k]
                sums_ref[tile] += products[k]
            return carry

        lax.fori_loop(0, (live + unroll - 1) // unroll, group, 0)


def vmem_left(held):
    return VMEM_BYTES - 4 * held - SPARE_BYTES


def deposit(block_count, block_tile, corner, offset, radius, emission, extinction, tiles_all):
    slots, lanes = radius.shape[1:]
    chunk = min(CHUNK, slots)
    unroll = min(UNROLL, chunk)

    def at(step, count_ref):
        return jnp.minimum(step, (count_ref[0, 0] - 1) // chunk)

    def wide(step, count_ref, tile_ref):
        return (0, 0, at(step, count_ref), 0)

    def narrow(step, count_ref, tile_ref):
        return (0, at(step, count_ref), 0)

    return pl.pallas_call(
        functools.partial(deposit_kernel, chunk, unroll),
        grid_spec=pltpu.PrefetchScalarGridSpec(
            num_scalar_prefetch=2,
            grid=(slots // chunk,),
            in_specs=[
                pl.BlockSpec((2, 1, chunk, lanes), wide),
                pl.BlockSpec((2, 1, chunk, lanes), wide),
                pl.BlockSpec((1, chunk, lanes), narrow),
                pl.BlockSpec((3, 1, chunk, lanes), wide),
                pl.BlockSpec((1, chunk, lanes), narrow),
            ],
            out_specs=pl.BlockSpec(memory_space=pltpu.VMEM),
            scratch_shapes=[
                pltpu.VMEM((2, chunk, lanes), jnp.float32),
                pltpu.VMEM((2, chunk, lanes), jnp.float32),
                pltpu.VMEM((4, chunk, lanes), jnp.float32),
            ],
        ),
        out_shape=pltpu.VMEM((tiles_all, TS, 4 * TS), jnp.float32),
        compiler_params=pltpu.CompilerParams(
            vmem_limit_bytes=vmem_left(tiles_all * TS * 4 * TS), dimension_semantics=("arbitrary",)),
        name="deposit",
    )(block_count, block_tile, corner, offset, radius, emission, extinction)


def signal(barrier, device):
    pl.semaphore_signal(barrier, inc=1, device_id=device, device_id_type=pl.DeviceIdType.MESH)


def exchange_kernel(rank_ref, partial_ref, image_ref, held_ref, stack_ref, ready_ref, landed_ref,
                    send_sem, recv_sem, out_sem, in_sem, image_send_sem, image_recv_sem, ready_sem):
    depth_size, screen_size, rows, lanes = partial_ref.shape
    half = screen_size // 2
    part = rows // CUTS
    pieces = half * depth_size * CUTS
    edge = (screen_size - 1, 0)
    me = lax.axis_index("screen")
    slab = lax.axis_index("depth")

    at_edge = jnp.logical_or(me == 0, me == screen_size - 1)
    middle = jnp.logical_not(at_edge)
    home = jnp.where(me < half, 0, screen_size - 1)
    beside = jnp.logical_or(me == 1, me == screen_size - 2)
    barrier = pltpu.get_barrier_semaphore()

    def greet(present, device):
        @pl.when(present)
        def _():
            signal(barrier, device)

    greet(me > 1, {"screen": me - 1})
    greet(me < screen_size - 2, {"screen": me + 1})
    for hop in range(1, depth_size):
        greet(at_edge, {"depth": lax.rem(slab + hop, depth_size)})
    greet(jnp.logical_and(middle, jnp.logical_not(beside)), {"screen": home})

    @pl.when(middle)
    def _():
        pl.semaphore_wait(barrier, 2)

    @pl.when(beside)
    def _():
        signal(ready_sem, {"screen": home})

    @pl.when(at_edge)
    def _():
        pl.semaphore_wait(ready_sem, 1)

    def place(side, j):
        stage = j // depth_size
        group = stage // CUTS
        target = lax.rem(slab + 1 + lax.rem(j, depth_size), depth_size)
        owner = jnp.where(side == 1, half - 1 - group, half + group)
        return group, target, owner, lax.rem(stage, CUTS)

    def rows_of(cut):
        return pl.ds(pl.multiple_of(cut * part, part), part)

    def hop(side, j, source):
        return pltpu.make_async_remote_copy(
            src_ref=source, dst_ref=held_ref.at[side, j],
            send_sem=send_sem.at[side], recv_sem=recv_sem.at[side, j],
            device_id={"screen": me + 1 - 2 * side}, device_id_type=pl.DeviceIdType.MESH)

    def across(side, j, group, target, cut):
        return pltpu.make_async_remote_copy(
            src_ref=held_ref.at[side, j], dst_ref=stack_ref.at[group, slab, rows_of(cut)],
            send_sem=out_sem, recv_sem=in_sem.at[group, cut],
            device_id={"depth": target}, device_id_type=pl.DeviceIdType.MESH)

    def handed(group, owner):
        return pltpu.make_async_remote_copy(
            src_ref=ready_ref.at[group], dst_ref=landed_ref,
            send_sem=image_send_sem.at[group], recv_sem=image_recv_sem,
            device_id={"screen": owner}, device_id_type=pl.DeviceIdType.MESH)

    for side in range(2):
        @pl.when(me == side * (screen_size - 1))
        def _(side=side):
            def launch(j, carry):
                group, target, owner, cut = place(side, j)
                hop(side, j, partial_ref.at[target, owner, rows_of(cut)]).start()
                return carry

            lax.fori_loop(0, pieces, launch, 0)

    @pl.when(middle)
    def _():
        lead = jnp.where(me < half, 0, 1)
        behind = LAG * jnp.abs(2 * me - (screen_size - 1))

        def forward(side, j):
            @pl.when(jnp.logical_and(j >= 0, j < pieces))
            def _():
                group, target, owner, cut = place(side, j)
                move = hop(side, j, held_ref.at[side, j])
                move.wait_recv()
                held_ref[side, j] += partial_ref[target, owner, rows_of(cut)]
                move.start()

        def relay(i, carry):
            forward(lead, i)
            forward(1 - lead, i - behind)
            return carry

        lax.fori_loop(0, pieces + LAG * (screen_size - 1), relay, 0)

    quarter = lanes // 4

    def composite(group, cut, out_ref):
        before = [[jnp.where(rank_ref[k] < rank_ref[j], 1.0, 0.0) for k in range(depth_size)]
                  for j in range(depth_size)]
        lane = lax.broadcasted_iota(jnp.int32, (TS, lanes), 1)
        optical_lane = lane >= 3 * quarter

        low_lane = lax.rem(lane, 2 * FOOT) < FOOT

        def whole_rows(k, index):
            near = stack_ref[group, k, pl.ds(pl.multiple_of(index * TS, TS), FOOT)]
            total = stack_ref[group, k, pl.ds(pl.multiple_of(index * TS + FOOT, FOOT), FOOT)]
            both = jnp.concatenate([near, total - near], 0)
            return both - jnp.where(low_lane, 0.0, pltpu.roll(both, FOOT, 1))

        def step(index, carry):
            now = pl.ds(pl.multiple_of(index * TS, TS), TS)
            slabs = [whole_rows(k, index) for k in range(depth_size)]
            depths = []
            for k in range(depth_size):
                optical = jnp.where(optical_lane, slabs[k], 0.0)
                optical = optical + pltpu.roll(optical, 2 * quarter, 1)
                depths.append(optical + pltpu.roll(optical, quarter, 1))
            lighting = jnp.zeros((TS, lanes), jnp.float32)
            for j in range(depth_size):
                reach = 0.5 * depths[j]
                for k in range(depth_size):
                    if k != j:
                        reach = reach + before[j][k] * depths[k]
                lighting = lighting + jnp.exp(-reach) * slabs[j]
            whole = depths[0]
            for k in range(1, depth_size):
                whole = whole + depths[k]
            out_ref[now] = jnp.where(optical_lane, 1.0 - jnp.exp(-whole), lighting)
            return carry

        lax.fori_loop(cut * (part // TS), (cut + 1) * (part // TS), step, 0)

    def gather(group, cut):
        arrived = stack_ref.at[group, pl.ds(0, depth_size - 1), rows_of(cut)]
        pltpu.make_async_remote_copy(
            src_ref=arrived, dst_ref=arrived, send_sem=out_sem, recv_sem=in_sem.at[group, cut],
            device_id={"depth": lax.rem(slab + 1, depth_size)},
            device_id_type=pl.DeviceIdType.MESH).wait_recv()

    for side in range(2):
        @pl.when(me == edge[side])
        def _(side=side):
            def collect(j, carry):
                group, target, owner, cut = place(side, j)
                hop(side, j, held_ref.at[side, j]).wait_recv()

                @pl.when(target != slab)
                def _():
                    held_ref[side, j] += partial_ref[target, owner, rows_of(cut)]
                    across(side, j, group, target, cut).start()

                @pl.when(target == slab)
                def _():
                    stack_ref[group, slab, rows_of(cut)] = (
                        held_ref[side, j] + partial_ref[target, owner, rows_of(cut)])
                return carry

            def finish(stage):
                group, cut = divmod(stage, CUTS)
                gather(group, cut)
                composite(group, cut, image_ref if group == half - 1 else ready_ref.at[group])
                if group < half - 1 and cut == CUTS - 1:
                    handed(group, half - 1 - group if side else half + group).start()

            pl.semaphore_wait(barrier, depth_size - 1 + max(half - 2, 0))
            for stage in range(half * CUTS):
                lax.fori_loop(stage * depth_size, (stage + 1) * depth_size, collect, 0)
                if stage > 0:
                    finish(stage - 1)
            finish(half * CUTS - 1)

            all_sent = held_ref.at[side, pl.ds(0, half * (depth_size - 1) * CUTS)]
            pltpu.make_async_remote_copy(
                src_ref=all_sent, dst_ref=all_sent, send_sem=out_sem, recv_sem=in_sem.at[0, 0],
                device_id={"depth": lax.rem(slab + 1, depth_size)},
                device_id_type=pl.DeviceIdType.MESH).wait_send()
            for group in range(half - 1):
                handed(group, half - 1 - group if side else half + group).wait_send()

    @pl.when(middle)
    def _():
        handed(0, me).wait_recv()
        image_ref[...] = landed_ref[...]

    for side in range(2):
        @pl.when(me != edge[side])
        def _(side=side):
            pltpu.make_async_remote_copy(
                src_ref=held_ref.at[side], dst_ref=held_ref.at[side],
                send_sem=send_sem.at[side], recv_sem=recv_sem.at[side, 0],
                device_id={"screen": me + 1 - 2 * side},
                device_id_type=pl.DeviceIdType.MESH).wait_send()


def exchange(partial_value, slab_rank):
    depth_size, screen_size, rows, lanes = partial_value.shape
    half = screen_size // 2
    pieces = half * depth_size * CUTS
    return pl.pallas_call(
        exchange_kernel,
        in_specs=[pl.BlockSpec(memory_space=pltpu.SMEM), pl.BlockSpec(memory_space=pltpu.VMEM)],
        out_specs=pl.BlockSpec(memory_space=pltpu.VMEM),
        out_shape=pltpu.VMEM((rows, lanes), jnp.float32),
        scratch_shapes=[
            pltpu.VMEM((2, pieces, rows // CUTS, lanes), jnp.float32),
            pltpu.VMEM((half, depth_size, rows, lanes), jnp.float32),
            pltpu.VMEM((max(half - 1, 1), rows, lanes), jnp.float32),
            pltpu.VMEM((rows, lanes), jnp.float32),
            pltpu.SemaphoreType.DMA((2,)),
            pltpu.SemaphoreType.DMA((2, pieces)),
            pltpu.SemaphoreType.DMA,
            pltpu.SemaphoreType.DMA((half, CUTS)),
            pltpu.SemaphoreType.DMA((max(half - 1, 1),)),
            pltpu.SemaphoreType.DMA,
            pltpu.SemaphoreType.REGULAR,
        ],
        compiler_params=pltpu.CompilerParams(
            vmem_limit_bytes=vmem_left(partial_value.size),
            collective_id=0, has_side_effects=True),
        name="exchange",
    )(slab_rank, pltpu.with_memory_space_constraint(partial_value, pltpu.VMEM))


def shards(block_tile, block_count, slab_rank, corner, offset, radius, emission, extinction):
    depth_size = lax.axis_size("depth")
    screen_size = lax.axis_size("screen")
    tiles_all = TILE_DEV * depth_size * screen_size
    partial_value = deposit(
        block_count, block_tile, corner, offset, radius, emission, extinction, tiles_all)
    gathered = partial_value.reshape(depth_size, screen_size, TILE_DEV * TS, 4 * TS)
    return exchange(gathered, slab_rank).reshape(TILE_DEV, TS, 4 * TS)


def solution(mesh):
    placed = (
        P("depth", "screen"),
        P("depth", "screen"),
        P(),
        P(None, "depth", "screen", None),
        P(None, "depth", "screen", None),
        P("depth", "screen", None),
        P(None, "depth", "screen", None),
        P("depth", "screen", None),
    )
    return jax.shard_map(
        shards,
        mesh=mesh,
        in_specs=placed,
        out_specs=P(("depth", "screen"), None, None),
        check_vma=False,
    )
```
